32 devices in a mesh: frame: 4 (over z), height: 4 (over y, x), dp: 2 (over core).
Axes of the slice: x: 2, y: 2, z: 4, core: 2. Of those that a mesh axis runs over, the one named last changes fastest.
Arguments:
- clip_latents: bfloat16 [2, 8, 64, 16, 320], P('dp', 'frame', 'height'), may hold values from -6 to 6
- out_grad: bfloat16 [2, 8, 64, 16, 320], P('dp', 'frame', 'height'), may hold values from -6 to 6
- box_mask: int32 [2, 8, 64, 16], P('dp', 'frame', 'height'), may hold values from 0 to 1, as said below
- attn_weights: bfloat16 [1280, 320], replicated, may hold values from -0.3125 to 0.3125
- conv_weights: bfloat16 [2880, 320], replicated, may hold values from -0.109375 to 0.109375
- time_bias: float32 [5, 8, 8], replicated, may hold values from -4 to 250
Outputs:
- grad_input: bfloat16 [2, 8, 64, 16, 320], P('dp', 'frame', 'height')
- grad_attn: float32 [1280, 320], P(('frame', 'height', 'dp'))
- grad_conv: float32 [2880, 320], P(('height', 'dp'))
The draws below stay inside these ranges and needn't reach their ends.
Inputs may be any that keep to these rules, and one draw needn't show every extreme that they name: Each frame of each clip has one grounding box: box_mask is 1 on a rectangle of 16 to 32 rows and 4 to 8 columns, 0 elsewhere.
All inputs are finite; a program needn't handle non-finite values.
Results may differ from the reference program's by a relative error of at most 0.025.
Values may be sent and summed in bfloat16 or wider, within the bound.
No kernel may reach another device: no remote copies, remote signals or barrier semaphores. Data moves between devices by JAX's collectives and lax.ppermute only.
A program may use at most 64 MiB of HBM per device.

```python
import jax
import jax.numpy as jnp
from jax import lax

HEADS = 5
C = 320
WID = 16
CLIPS = 2
FRAMES = 8
HGT = 64


def draw_box_mask(key, part):
    keys = jax.random.split(jax.random.fold_in(key, 11), 4)
    shape = (CLIPS, FRAMES)
    box_top = jax.random.randint(keys[0], shape, 0, HGT // 2)
    box_tall = jax.random.randint(keys[1], shape, HGT // 4, HGT // 2 + 1)
    box_left = jax.random.randint(keys[2], shape, 0, WID // 2)
    box_wide = jax.random.randint(keys[3], shape, WID // 4, WID // 2 + 1)
    row_ids = jnp.arange(HGT)[None, None, :]
    col_ids = jnp.arange(WID)[None, None, :]
    inside_rows = (row_ids >= box_top[..., None]) & (row_ids < (box_top + box_tall)[..., None])
    inside_cols = (col_ids >= box_left[..., None]) & (col_ids < (box_left + box_wide)[..., None])
    inside = inside_rows[..., :, None] & inside_cols[..., None, :]
    return inside.astype(jnp.int32)


def draw_time_bias(key, part):
    keys = jax.random.split(jax.random.fold_in(key, 23), 1)
    shape = (HEADS, FRAMES, FRAMES)
    values = jnp.clip(jax.random.normal(keys[0], shape, jnp.float32), -4.0, 4.0)
    return values.astype(jnp.float32)


def shard_levels(stream_key, dims, cuts, least, largest):
    loudness = 1.0
    for axis_at, blocks in cuts:
        draws = jax.random.uniform(jax.random.fold_in(jax.random.fold_in(stream_key, 6), axis_at), (blocks,), jnp.float32, least / len(cuts), largest / len(cuts))
        loudness = loudness * jnp.repeat(jnp.exp(draws), dims[axis_at] // blocks).reshape((-1,) + (1,) * (len(dims) - 1 - axis_at))
    return loudness


def bell_draw(rng, dims, width, limit, shards=(), dtype=jnp.bfloat16):
    gain = shard_levels(rng, dims, shards, -0.22, 0.18) if shards else 1.0
    array = jax.random.normal(rng, dims, jnp.float32) * width * gain
    return jnp.minimum(jnp.maximum(array, -limit), limit).astype(dtype)


def setup_inputs(seed: int = 0) -> dict:
    splits = jax.random.split(jax.random.key(seed), 7)
    clip_latents = bell_draw(splits[0], (CLIPS, FRAMES, HGT, WID, C), 1.0, 6.0, ((0, 2), (1, 4), (2, 4)))
    out_grad = bell_draw(splits[1], (CLIPS, FRAMES, HGT, WID, C), 1.0, 6.0, ((0, 2), (1, 4), (2, 4)))
    box_mask = draw_box_mask(jax.random.fold_in(splits[6], 71), 0)
    attn_weights = bell_draw(splits[3], (4 * C, C), C ** -0.5, 0.3125)
    conv_weights = bell_draw(splits[4], (9 * C, C), (9 * C) ** -0.5, 0.109375)
    time_bias = draw_time_bias(jax.random.fold_in(splits[6], 71), 0)
    return {"clip_latents": clip_latents, "out_grad": out_grad, "box_mask": box_mask, "attn_weights": attn_weights, "conv_weights": conv_weights, "time_bias": time_bias}


ground_bias = 2.0


def silu_slope(value):
    sig = jax.nn.sigmoid(value)
    return sig * (1.0 + value * (1.0 - sig))


def matmul(left, right):
    return jnp.dot(left, right, preferred_element_type=jnp.float32)


def one_clip(inputs, attn_weights, conv_weights, time_bias):
    latents, upstream_grad, marks = inputs
    frame_count, row_count, col_count, channels = latents.shape
    pixels = row_count * col_count
    head_size = channels // HEADS
    scaling = head_size ** -0.5
    w_query = attn_weights[:channels]
    w_key = attn_weights[channels:2 * channels]
    w_value = attn_weights[2 * channels:3 * channels]
    w_out = attn_weights[3 * channels:]
    flat_x = latents.reshape(-1, channels)
    query_rows = matmul(flat_x, w_query).astype(jnp.bfloat16)
    key_rows = matmul(flat_x, w_key).astype(jnp.bfloat16)
    value_rows = matmul(flat_x, w_value).astype(jnp.bfloat16)
    head_shape = (frame_count, pixels, HEADS, head_size)
    qh = query_rows.reshape(head_shape).astype(jnp.float32)
    kh = key_rows.reshape(head_shape).astype(jnp.float32)
    vh = value_rows.reshape(head_shape).astype(jnp.float32)
    mark_bias = ground_bias * marks.reshape(frame_count, pixels).T.astype(jnp.float32)
    scores = jnp.einsum("tnhd,unhd->nhtu", qh, kh) * scaling + time_bias[None] + mark_bias[:, None, None, :]
    prob_full = jax.nn.softmax(scores, axis=-1)
    prob_half = prob_full.astype(jnp.bfloat16)
    mixed_rows = jnp.einsum("nhtu,unhd->tnhd", prob_half.astype(jnp.float32), vh).astype(jnp.bfloat16).reshape(-1, channels)
    residual = (flat_x.astype(jnp.float32) + matmul(mixed_rows, w_out)).astype(jnp.bfloat16)
    activated = jax.nn.silu(residual.astype(jnp.float32)).astype(jnp.bfloat16)
    image_shape = (frame_count, row_count, col_count, channels)
    widths = ((0, 0), (1, 1), (1, 1), (0, 0))
    act_pad = jnp.pad(activated.reshape(image_shape), widths)
    grad_pad = jnp.pad(upstream_grad, widths)
    out_rows = upstream_grad.reshape(-1, channels)
    delta_sum = jnp.zeros((frame_count * pixels, channels), jnp.float32)
    conv_terms = []
    for row_step in (-1, 0, 1):
        for col_step in (-1, 0, 1):
            tap_index = 3 * (row_step + 1) + col_step + 1
            tap_weight = conv_weights[tap_index * channels:(tap_index + 1) * channels]
            shifted = grad_pad[:, 1 - row_step:1 - row_step + row_count, 1 - col_step:1 - col_step + col_count, :]
            delta_sum = delta_sum + matmul(shifted.reshape(-1, channels), tap_weight.T)
            moved_rows = act_pad[:, 1 + row_step:1 + row_step + row_count, 1 + col_step:1 + col_step + col_count, :]
            conv_terms.append(matmul(moved_rows.reshape(-1, channels).T, out_rows))
    upstream = (out_rows.astype(jnp.float32) + silu_slope(residual.astype(jnp.float32)) * delta_sum).astype(jnp.bfloat16)
    d_mixed = matmul(upstream, w_out.T).astype(jnp.bfloat16)
    dh = d_mixed.reshape(head_shape).astype(jnp.float32)
    d_prob = jnp.einsum("tnhd,unhd->nhtu", dh, vh)
    row_dot = jnp.sum(prob_full * d_prob, axis=-1, keepdims=True)
    d_scores = (prob_full * (d_prob - row_dot)).astype(jnp.bfloat16).astype(jnp.float32)
    d_query = (jnp.einsum("nhtu,unhd->tnhd", d_scores, kh) * scaling).astype(jnp.bfloat16).reshape(-1, channels)
    d_key = (jnp.einsum("nhtu,tnhd->unhd", d_scores, qh) * scaling).astype(jnp.bfloat16).reshape(-1, channels)
    d_value = jnp.einsum("nhtu,tnhd->unhd", prob_half.astype(jnp.float32), dh).astype(jnp.bfloat16).reshape(-1, channels)
    d_inputs = (matmul(d_query, w_query.T) + matmul(d_key, w_key.T) + matmul(d_value, w_value.T)).astype(jnp.bfloat16)
    grad_rows = (upstream.astype(jnp.float32) + d_inputs.astype(jnp.float32)).astype(jnp.bfloat16)
    attn_term = jnp.concatenate([matmul(flat_x.T, d_query), matmul(flat_x.T, d_key), matmul(flat_x.T, d_value), matmul(mixed_rows.T, upstream)], axis=0)
    conv_term = jnp.concatenate(conv_terms, axis=0)
    return grad_rows.reshape(image_shape), attn_term, conv_term


def reference(clip_latents, out_grad, box_mask, attn_weights, conv_weights, time_bias):
    grad_input, attn_terms, conv_terms = lax.map(
        lambda inputs: one_clip(inputs, attn_weights, conv_weights, time_bias),
        (clip_latents, out_grad, box_mask))
    grad_scale = (CLIPS * FRAMES * HGT * WID) ** -0.5
    grad_attn = jnp.sum(attn_terms, axis=0) * grad_scale
    grad_conv = jnp.sum(conv_terms, axis=0) * grad_scale
    return grad_input, grad_attn, grad_conv
```

```python
import functools

import jax
import jax.numpy as jnp
from jax import lax
from jax.experimental import pallas as pl
from jax.experimental.pallas import tpu as pltpu
from jax.sharding import PartitionSpec as P


ground_bias = 2.0
LANES = 128
BF = jnp.bfloat16
F32 = jnp.float32


def dot(left, right, dims=((1,), (0,))):
    return lax.dot_general(left, right, (dims, ((), ())), preferred_element_type=F32)


def is_pow2(count):
    return count & (count - 1) == 0


def peer(index, step, count):
    if is_pow2(count):
        return index ^ step
    return (step - index) % count


def trade(value, axis, step):
    count = lax.axis_size(axis)
    return lax.ppermute(value, axis, [(i, peer(i, step, count)) for i in range(count)])


def own_step(index, count):
    if is_pow2(count):
        return 0
    raise NotImplementedError("axis size")


def sigmoid(value):
    return 1.0 / (1.0 + jnp.exp(-value))


def merge_rows(value):
    return value.reshape(-1, value.shape[-1])


def head_tiles(channels, head_size):
    step = max(LANES, head_size)
    tiles = []
    for start in range(0, channels, step):
        width = min(step, channels - start)
        tiles.append((start, width, range(start // head_size, (start + width) // head_size)))
    return tiles


def head_mask(tokens, width, head_size, place):
    lane = lax.broadcasted_iota(jnp.int32, (tokens, width), 1)
    return lane // head_size == place


def forward_kernel(parts, channels, head_size, *refs):
    x_refs = refs[:parts]
    w_ref, bias_ref = refs[parts : parts + 2]
    q_ref, k_ref, v_ref, p_ref, o_ref, y_ref, a_ref = refs[parts + 2 :]
    frames, rows, cols, _ = q_ref.shape
    tokens = frames * cols
    wide = jnp.concatenate([merge_rows(ref[...]) for ref in x_refs], axis=0)
    latents = wide[:, :channels]
    for place, ref in enumerate((q_ref, k_ref, v_ref)):
        part = dot(latents, w_ref[place * channels : (place + 1) * channels, :]).astype(BF)
        ref[...] = part.reshape(ref.shape)
    scaling = head_size ** (-0.5)
    spare = (channels // LANES) * LANES
    tile_row = lax.broadcasted_iota(jnp.int32, (LANES, tokens), 0)
    tile_col = lax.broadcasted_iota(jnp.int32, (LANES, tokens), 1)
    pick = jnp.where(tile_row - (channels - spare) == tile_col % cols, ground_bias, 0.0).astype(BF)
    marks = dot(wide[:, spare : spare + LANES], pick).reshape(frames, rows, cols, tokens)
    for row in range(rows):
        mark = marks[:, row].reshape(tokens, tokens)
        for start, width, heads in head_tiles(channels, head_size):
            lanes = slice(start, start + width)
            q_tile = q_ref[:, row, :, lanes].reshape(tokens, width)
            k_tile = k_ref[:, row, :, lanes].reshape(tokens, width)
            v_tile = v_ref[:, row, :, lanes].reshape(tokens, width)
            mixed = None
            for place, head in enumerate(heads):
                mask = head_mask(tokens, width, head_size, place)
                q_head = q_tile * mask.astype(BF) if len(heads) > 1 else q_tile
                score = dot(k_tile, q_head, ((1,), (1,))) * scaling + (bias_ref[head] + mark)
                score = jnp.exp(score - jnp.max(score, axis=0, keepdims=True))
                prob = score * (1.0 / jnp.sum(score, axis=0, keepdims=True))
                p_ref[row, head] = prob
                out = dot(prob.astype(BF), v_tile, ((0,), (0,)))
                mixed = out if mixed is None else jnp.where(mask, out, mixed)
            o_ref[:, row, :, lanes] = mixed.astype(BF).reshape(frames, cols, width)
    mixed = merge_rows(o_ref[...])
    residual = (latents.astype(F32) + dot(mixed, w_ref[3 * channels :, :])).astype(BF)
    y_ref[...] = residual.reshape(y_ref.shape)
    value = residual.astype(F32)
    a_ref[...] = (value * sigmoid(value)).astype(BF).reshape(a_ref.shape)


def column_moves(dy_refs, rows, cols):
    whole = jnp.concatenate([ref[...] for ref in dy_refs], axis=0)
    shape = whole.shape
    flat = merge_rows(whole)
    count = flat.shape[0]
    wide = flat.astype(F32)
    col = lax.broadcasted_iota(jnp.int32, wide.shape, 0) % cols
    right = jnp.where(col == 0, 0.0, pltpu.roll(wide, 1, 0)).astype(BF)
    left = jnp.where(col == cols - 1, 0.0, pltpu.roll(wide, count - 1, 0)).astype(BF)
    return left.reshape(shape), whole, right.reshape(shape)


def tap_of(moves, row_step, col_step, rows):
    return merge_rows(moves[col_step + 1][:, 1 - row_step : 1 - row_step + rows])


def write_blocks(total_ref, keep_ref, send_ref, height, frame, dp, split):
    if split is None:
        keep_ref[...] = total_ref[...].astype(BF)
        return
    frame_count, height_count, dp_count, size = split
    for high in range(height_count):
        for far in range(frame_count):
            owner = ((frame ^ far) * height_count + (height ^ high)) * dp_count
            for ref, side in ((keep_ref, dp), (send_ref, 1 - dp)):
                first = pl.multiple_of((owner + side) * size, 8)
                ref[high, far] = total_ref[pl.ds(first, size), :].astype(BF)


def conv_grad_kernel(parts, grad_scale, split, *refs):
    place_ref = refs[0]
    dy_refs = refs[1 : 1 + parts]
    a_ref, keep_ref, send_ref, total_ref = refs[1 + parts :]
    frames, rows, cols, channels = a_ref.shape
    moves = column_moves(dy_refs, rows, cols)
    act = merge_rows(a_ref[...]).T
    for tap in range(9):
        moved = tap_of(moves, tap // 3 - 1, tap % 3 - 1, rows)
        total_ref[tap * channels : (tap + 1) * channels, :] = dot(act, moved) * grad_scale
    write_blocks(total_ref, keep_ref, send_ref, place_ref[1], 0, place_ref[2], split)


def backward_kernel(parts, channels, head_size, grad_scale, split, *refs):
    place_ref = refs[0]
    dy_refs = refs[1 : 1 + parts]
    x_refs = refs[1 + parts : 1 + 2 * parts]
    (y_ref, q_ref, k_ref, v_ref, p_ref, o_ref, w_ref, conv_ref) = refs[1 + 2 * parts : 9 + 2 * parts]
    out_refs = refs[9 + 2 * parts : 9 + 3 * parts]
    keep_ref, send_ref, do_ref, dq_ref, dk_ref, dv_ref, total_ref = refs[9 + 3 * parts :]
    frames, rows, cols, _ = q_ref.shape
    tokens = frames * cols
    scaling = head_size ** (-0.5)
    moves = column_moves(dy_refs, rows, cols)
    delta = None
    for tap in range(9):
        moved = tap_of(moves, tap // 3 - 1, tap % 3 - 1, rows)
        term = dot(moved, conv_ref[tap * channels : (tap + 1) * channels, :], ((1,), (1,)))
        delta = term if delta is None else delta + term
    value = merge_rows(y_ref[...]).astype(F32)
    sig = sigmoid(value)
    slope = sig * (1.0 + value * (1.0 - sig))
    dy = tap_of(moves, 0, 0, rows).astype(F32)
    upstream = (dy + slope * delta).astype(BF)
    w_out = w_ref[3 * channels :, :]
    total_ref[3 * channels :, :] = dot(merge_rows(o_ref[...]).T, upstream) * grad_scale
    do_ref[...] = dot(upstream, w_out, ((1,), (1,))).astype(BF).reshape(do_ref.shape)
    for row in range(rows):
        for start, width, heads in head_tiles(channels, head_size):
            lanes = slice(start, start + width)
            q_tile = q_ref[:, row, :, lanes].reshape(tokens, width)
            k_tile = k_ref[:, row, :, lanes].reshape(tokens, width)
            v_tile = v_ref[:, row, :, lanes].reshape(tokens, width)
            do_tile = do_ref[:, row, :, lanes].reshape(tokens, width)
            dq = dk = dv = None
            for place, head in enumerate(heads):
                mask = head_mask(tokens, width, head_size, place)
                do_head = do_tile * mask.astype(BF) if len(heads) > 1 else do_tile
                prob = p_ref[row, head]
                d_prob = dot(v_tile, do_head, ((1,), (1,)))
                row_dot = jnp.sum(prob * d_prob, axis=0, keepdims=True)
                d_score = (prob * (d_prob - row_dot)).astype(BF)
                terms = (
                    dot(d_score, k_tile, ((0,), (0,))),
                    dot(d_score, q_tile),
                    dot(prob.astype(BF), do_tile),
                )
                if dq is None:
                    dq, dk, dv = terms
                else:
                    dq, dk, dv = (
                        jnp.where(mask, new, old) for new, old in zip(terms, (dq, dk, dv))
                    )
            for ref, grad in ((dq_ref, dq * scaling), (dk_ref, dk * scaling), (dv_ref, dv)):
                ref[:, row, :, lanes] = grad.astype(BF).reshape(frames, cols, width)
    latents = jnp.concatenate([merge_rows(ref[...])[:, :channels] for ref in x_refs], axis=0)
    turned = latents.T
    d_inputs = None
    for place, ref in enumerate((dq_ref, dk_ref, dv_ref)):
        grad = merge_rows(ref[...])
        block = slice(place * channels, (place + 1) * channels)
        term = dot(grad, w_ref[block, :], ((1,), (1,)))
        d_inputs = term if d_inputs is None else d_inputs + term
        total_ref[block, :] = dot(turned, grad) * grad_scale
    grads = (upstream.astype(F32) + d_inputs.astype(BF).astype(F32)).astype(BF)
    share = grads.shape[0] // parts
    for step, ref in enumerate(out_refs):
        ref[...] = grads[step * share : (step + 1) * share].reshape(ref.shape)
    write_blocks(total_ref, keep_ref, send_ref, place_ref[1], place_ref[0], place_ref[2], split)


def place_kernel(parts, *refs):
    place_ref = refs[0]
    part_refs = refs[1 : 1 + parts]
    out_ref = refs[1 + parts]
    rows = part_refs[0].shape[1]
    for step, ref in enumerate(part_refs):
        out_ref[:, pl.ds((place_ref[0] ^ step) * rows, rows)] = ref[...]


def call(kernel, outs, args, scratch=(), scalars=False, flops=0):
    vmem = pl.BlockSpec(memory_space=pltpu.VMEM)
    smem = pl.BlockSpec(memory_space=pltpu.SMEM)
    specs = [vmem] * len(args)
    if scalars:
        specs[0] = smem
    moved = sum(v.size * v.dtype.itemsize for v in list(args) + list(outs))
    return pl.pallas_call(
        kernel,
        out_shape=outs,
        in_specs=specs,
        out_specs=[vmem] * len(outs),
        scratch_shapes=list(scratch),
        cost_estimate=pl.CostEstimate(flops=flops, transcendentals=0, bytes_accessed=moved),
        compiler_params=pltpu.CompilerParams(vmem_limit_bytes=56 * 1024 * 1024),
    )(*args)


def block_size(total, owners):
    size = total // owners
    return size if size % 8 == 0 else None


def pack_blocks(plain, frame_count, height_count, dp_count, me, high, side):
    blocks = plain.reshape(frame_count, height_count, dp_count, -1, plain.shape[-1])
    far = jnp.arange(frame_count) ^ (me if frame_count > 1 else 0)
    blocks = blocks[far][:, jnp.arange(height_count) ^ high]
    blocks = jnp.swapaxes(blocks, 0, 1)
    keep = lax.dynamic_index_in_dim(blocks, side, 2, keepdims=False)
    send = lax.dynamic_index_in_dim(blocks, 1 - side, 2, keepdims=False)
    return keep, send


def reduce_local(keep, send):
    got = lax.ppermute(send, "dp", [(0, 1), (1, 0)])
    both = (keep.astype(F32) + got.astype(F32)).astype(BF)
    total = both[0].astype(F32)
    for value in [trade(both[step], "height", step) for step in range(1, keep.shape[0])]:
        total = total + value.astype(F32)
    return total


def body(clip_latents, out_grad, box_mask, attn_weights, conv_weights, time_bias):
    clips, frame_count, row_count, cols, channels = clip_latents.shape
    head_count, all_frames, _ = time_bias.shape
    head_size = channels // head_count
    parts = lax.axis_size("frame")
    height_count = lax.axis_size("height")
    dp_count = lax.axis_size("dp")
    me = lax.axis_index("frame")
    high = lax.axis_index("height")
    side = lax.axis_index("dp")
    rows = row_count // parts
    assert clips == 1 and dp_count == 2 and rows * parts == row_count
    assert is_pow2(parts) and is_pow2(height_count)
    tokens = all_frames * cols
    place = jnp.stack([me, high, side]).astype(jnp.int32)

    x = clip_latents[0]
    dy = out_grad[0]
    spare = -channels % LANES
    assert cols <= spare
    marks = jnp.broadcast_to(
        box_mask[0].astype(BF)[:, :, None, :], (frame_count, row_count, cols, cols)
    )
    blank = jnp.zeros((frame_count, row_count, cols, spare - cols), BF)
    wide = jnp.concatenate([x, marks, blank], axis=-1)
    x_parts = [lax.dynamic_slice_in_dim(wide, me * rows, rows, axis=1)]
    for step in range(1, parts):
        block = lax.dynamic_slice_in_dim(wide, (me ^ step) * rows, rows, axis=1)
        x_parts.append(trade(block, "frame", step))

    up = [(i, i + 1) for i in range(height_count - 1)]
    down = [(i + 1, i) for i in range(height_count - 1)]
    low = lax.ppermute(dy[:, -1:], "height", up)
    top = lax.ppermute(dy[:, :1], "height", down)
    padded = jnp.concatenate([low, dy, top], axis=1)
    dy_parts = [lax.dynamic_slice_in_dim(padded, me * rows, rows + 2, axis=1)]
    for step in range(1, parts):
        block = lax.dynamic_slice_in_dim(padded, (me ^ step) * rows, rows + 2, axis=1)
        dy_parts.append(trade(block, "frame", step))

    slot = jnp.arange(tokens)
    slot_frame = ((slot // (cols * frame_count)) ^ me) * frame_count + (slot // cols) % frame_count
    one_hot = (slot_frame[:, None] == jnp.arange(all_frames)[None, :]).astype(F32)
    spread = jnp.einsum(
        "au,htu,bt->hab", one_hot, time_bias, one_hot, precision=lax.Precision.HIGHEST
    )
    same = (slot[:, None] % cols) == (slot[None, :] % cols)
    bias = jnp.where(same[None], spread, -1e30)

    column = (all_frames, rows, cols, channels)
    half = jax.ShapeDtypeStruct(column, BF)
    probs = jax.ShapeDtypeStruct((rows, head_count, tokens, tokens), F32)
    pixels = all_frames * rows * cols
    q, k, v, p, o, y, a = call(
        functools.partial(forward_kernel, parts, channels, head_size),
        [half, half, half, probs, half, half, half],
        x_parts + [attn_weights, bias],
        flops=8 * pixels * channels * channels,
    )

    token_count = pixels * dp_count * parts * height_count
    grad_scale = float(token_count) ** (-0.5)

    def block_outs(total, frames):
        size = block_size(total, frames * height_count * dp_count)
        if size is None:
            return None, [
                jax.ShapeDtypeStruct((total, channels), BF),
                jax.ShapeDtypeStruct((8, channels), BF),
            ]
        shape = jax.ShapeDtypeStruct((height_count, frames, size, channels), BF)
        return (frames, height_count, dp_count, size), [shape, shape]

    taps = conv_weights.shape[0]
    split, outs = block_outs(taps, 1)
    keep, send = call(
        functools.partial(conv_grad_kernel, parts, grad_scale, split),
        outs,
        [place] + dy_parts + [a],
        scratch=[pltpu.VMEM((taps, channels), F32)],
        scalars=True,
        flops=2 * pixels * taps * channels,
    )
    if split is None:
        keep, send = pack_blocks(keep, 1, height_count, dp_count, 0, high, side)
    conv_sum = reduce_local(keep, send)[0]

    split, outs = block_outs(4 * channels, parts)
    piece = jax.ShapeDtypeStruct((frame_count, rows, cols, channels), BF)
    result = call(
        functools.partial(backward_kernel, parts, channels, head_size, grad_scale, split),
        [piece] * parts + outs,
        [place] + dy_parts + x_parts + [y, q, k, v, p, o, attn_weights, conv_weights],
        scratch=[pltpu.VMEM(column, BF)] * 4 + [pltpu.VMEM((4 * channels, channels), F32)],
        scalars=True,
        flops=2 * pixels * taps * channels,
    )
    grad_parts = [result[0]]
    for step in range(1, parts):
        grad_parts.append(trade(result[step], "frame", step))
    keep, send = result[parts:]
    if split is None:
        keep, send = pack_blocks(keep, parts, height_count, dp_count, me, high, side)
    attn_sum = reduce_local(keep, send).astype(BF)
    grad_attn = attn_sum[0].astype(F32)
    for step in range(1, parts):
        grad_attn = grad_attn + trade(attn_sum[step], "frame", step).astype(F32)

    size, _ = conv_sum.shape
    share = -(-size // (parts * 8)) * 8
    filled = jnp.pad(conv_sum, ((0, share * parts - size), (0, 0))).astype(BF)
    mine = lax.dynamic_slice_in_dim(filled, me * share, share, axis=0).astype(F32)
    for step in range(1, parts):
        block = lax.dynamic_slice_in_dim(filled, (me ^ step) * share, share, axis=0)
        mine = mine + trade(block, "frame", step).astype(F32)
    mine = mine.astype(BF)
    grad_conv = jnp.zeros((parts * share, channels), F32)
    for step in range(parts):
        block = mine if step == 0 else trade(mine, "frame", step)
        grad_conv = lax.dynamic_update_slice_in_dim(
            grad_conv, block.astype(F32), (me ^ step) * share, axis=0
        )
    grad_conv = grad_conv[:size]

    grad_input = call(
        functools.partial(place_kernel, parts),
        [jax.ShapeDtypeStruct((frame_count, row_count, cols, channels), BF)],
        [place] + grad_parts,
        scalars=True,
    )[0]
    return (grad_input.reshape(clip_latents.shape), grad_attn, grad_conv)


def solution(mesh):
    in_specs = (
        P("dp", "frame", "height", None, None),
        P("dp", "frame", "height", None, None),
        P("dp", "frame", "height", None),
        P(),
        P(),
        P(),
    )
    out_specs = (
        P("dp", "frame", "height", None, None),
        P(("frame", "height", "dp"), None),
        P(("height", "dp"), None),
    )
    return jax.shard_map(body, mesh=mesh, in_specs=in_specs, out_specs=out_specs, check_vma=False)
```

```python
import functools

import jax
import jax.numpy as jnp
from jax import lax
from jax.experimental import pallas as pl
from jax.experimental.pallas import tpu as pltpu
from jax.sharding import PartitionSpec as P


ground_bias = 2.0
LANES = 128
BF = jnp.bfloat16
F32 = jnp.float32


def dot(left, right, dims=((1,), (0,))):
    return lax.dot_general(left, right, (dims, ((), ())), preferred_element_type=F32)


def is_pow2(count):
    return count & (count - 1) == 0


def peer(index, step, count):
    if is_pow2(count):
        return index ^ step
    return (step - index) % count


def trade(value, axis, step):
    count = lax.axis_size(axis)
    return lax.ppermute(value, axis, [(i, peer(i, step, count)) for i in range(count)])


def sigmoid(value):
    return 1.0 / (1.0 + jnp.exp(-value))


def merge_rows(value):
    return value.reshape(-1, value.shape[-1])


def head_tiles(channels, head_size):
    step = max(LANES, head_size)
    tiles = []
    for start in range(0, channels, step):
        width = min(step, channels - start)
        tiles.append((start, width, range(start // head_size, (start + width) // head_size)))
    return tiles


def head_mask(tokens, width, head_size, place):
    lane = lax.broadcasted_iota(jnp.int32, (tokens, width), 1)
    return lane // head_size == place


def stack_heads(tile, heads, head_size):
    if len(heads) == 1:
        return tile
    masks = [head_mask(*tile.shape, head_size, place) for place in range(len(heads))]
    return jnp.concatenate([tile * mask.astype(BF) for mask in masks], axis=0)


def pick_heads(stacked, heads, head_size):
    tokens = stacked.shape[0] // len(heads)
    result = stacked[:tokens]
    for place in range(1, len(heads)):
        mask = head_mask(tokens, stacked.shape[1], head_size, place)
        result = jnp.where(mask, stacked[place * tokens : (place + 1) * tokens], result)
    return result


def tile_of(ref, row, lanes):
    frames, _, cols, _ = ref.shape
    return ref[:, row, :, lanes].reshape(frames * cols, lanes.stop - lanes.start)


def forward_kernel(parts, channels, head_size, *refs):
    x_refs = refs[:parts]
    w_ref, bias_ref = refs[parts : parts + 2]
    q_ref, k_ref, v_ref, p_ref, o_ref, y_ref, a_ref, s_ref = refs[parts + 2 :]
    frames, rows, cols, _ = q_ref.shape
    tokens = frames * cols
    head_count = channels // head_size
    wide = jnp.concatenate([merge_rows(ref[...]) for ref in x_refs], axis=0)
    latents = wide[:, :channels]
    for place, ref in enumerate((q_ref, k_ref, v_ref)):
        block = slice(place * channels, (place + 1) * channels)
        part = dot(latents, w_ref[:, block], ((1,), (1,))).astype(BF)
        ref[...] = part.reshape(ref.shape)
    scaling = head_size ** (-0.5)
    spare = (channels // LANES) * LANES
    tile_row = lax.broadcasted_iota(jnp.int32, (LANES, tokens), 0)
    tile_col = lax.broadcasted_iota(jnp.int32, (LANES, tokens), 1)
    pick = jnp.where(tile_row - (channels - spare) == tile_col % cols, ground_bias, 0.0).astype(BF)
    marks = dot(wide[:, spare : spare + LANES], pick).reshape(frames, rows, cols, tokens)
    tiles = head_tiles(channels, head_size)
    for row in range(rows):
        for start, width, heads in tiles:
            lanes = slice(start, start + width)
            queries = stack_heads(tile_of(q_ref, row, lanes), heads, head_size)
            span = slice(heads[0] * tokens, (heads[-1] + 1) * tokens)
            s_ref[row, :, span] = dot(tile_of(k_ref, row, lanes), queries, ((1,), (1,)))
    for row in range(rows):
        mark = marks[:, row].reshape(tokens, tokens)
        for head in range(head_count):
            span = slice(head * tokens, (head + 1) * tokens)
            score = s_ref[row, :, span] * scaling + (bias_ref[:, span] + mark)
            score = jnp.exp(score - jnp.max(score, axis=0, keepdims=True))
            p_ref[row, :, span] = score * (1.0 / jnp.sum(score, axis=0, keepdims=True))
    for row in range(rows):
        for start, width, heads in tiles:
            lanes = slice(start, start + width)
            span = slice(heads[0] * tokens, (heads[-1] + 1) * tokens)
            out = dot(p_ref[row, :, span].astype(BF), tile_of(v_ref, row, lanes), ((0,), (0,)))
            mixed = pick_heads(out, heads, head_size).astype(BF)
            o_ref[:, row, :, lanes] = mixed.reshape(frames, cols, width)
    mixed = merge_rows(o_ref[...])
    residual = (latents.astype(F32) + dot(mixed, w_ref[:, 3 * channels :], ((1,), (1,)))).astype(BF)
    y_ref[...] = residual.reshape(y_ref.shape)
    value = residual.astype(F32)
    a_ref[...] = (value * sigmoid(value)).astype(BF).reshape(a_ref.shape)


def column_moves(me, dy_refs, edge_refs, move_ref, cols):
    blocks = []
    for ref, edge_ref in zip(dy_refs, edge_refs):
        edge = edge_ref[...]
        first = jnp.where(me == 0, edge, ref[:, :1])
        last = jnp.where(me == len(dy_refs) - 1, edge, ref[:, -1:])
        blocks.append(jnp.concatenate([first, ref[:, 1:-1], last], axis=1))
    whole = jnp.concatenate(blocks, axis=0)
    wide = merge_rows(whole).astype(F32)
    count = wide.shape[0]
    col = lax.broadcasted_iota(jnp.int32, wide.shape, 0) % cols
    left = jnp.where(col == cols - 1, 0.0, pltpu.roll(wide, count - 1, 0))
    right = jnp.where(col == 0, 0.0, pltpu.roll(wide, 1, 0))
    move_ref[0] = left.astype(BF).reshape(whole.shape)
    move_ref[1] = whole
    move_ref[2] = right.astype(BF).reshape(whole.shape)


def tap_of(moves, row_step, col_step, rows):
    return merge_rows(moves[col_step + 1, :, 1 - row_step : 1 - row_step + rows])


def write_blocks(total_ref, keep_ref, send_ref, place_ref, split, turn=False):
    if split is None:
        keep_ref[...] = total_ref[...].astype(BF)
        return
    frame_count, height_count, dp_count, size = split
    for step in range(height_count):
        for far in range(frame_count):
            owner = (place_ref[0] ^ far) if frame_count > 1 else 0
            owner = (owner * height_count + (place_ref[1] ^ step)) * dp_count
            for ref, side in ((keep_ref, place_ref[2]), (send_ref, 1 - place_ref[2])):
                first = pl.multiple_of((owner + side) * size, 8)
                block = total_ref[pl.ds(first, size), :]
                if turn:
                    ref[step] = block.T.astype(BF)
                else:
                    ref[step, far] = block.astype(BF)


def conv_grad_kernel(parts, grad_scale, split, *refs):
    place_ref = refs[0]
    dy_refs = refs[1 : 1 + parts]
    edge_refs = refs[1 + parts : 1 + 2 * parts]
    a_ref, keep_ref, send_ref, move_ref, total_ref = refs[1 + 2 * parts :]
    _, rows, cols, channels = a_ref.shape
    column_moves(place_ref[0], dy_refs, edge_refs, move_ref, cols)
    act = merge_rows(a_ref[...]).T
    for tap in range(9):
        moved = tap_of(move_ref, tap // 3 - 1, tap % 3 - 1, rows)
        total_ref[tap * channels : (tap + 1) * channels, :] = dot(act, moved) * grad_scale
    write_blocks(total_ref, keep_ref, send_ref, place_ref, split, turn=True)


def upstream_kernel(channels, grad_scale, *refs):
    moves, y_ref, o_ref, w_ref, conv_ref, g_ref, do_ref, mix_ref = refs
    rows = g_ref.shape[1]
    delta = None
    for tap in range(9):
        moved = tap_of(moves, tap // 3 - 1, tap % 3 - 1, rows)
        term = dot(moved, conv_ref[:, tap * channels : (tap + 1) * channels])
        delta = term if delta is None else delta + term
    value = merge_rows(y_ref[...]).astype(F32)
    sig = sigmoid(value)
    slope = sig * (1.0 + value * (1.0 - sig))
    dy = tap_of(moves, 0, 0, rows).astype(F32)
    upstream = (dy + slope * delta).astype(BF)
    g_ref[...] = upstream.reshape(g_ref.shape)
    back = dot(upstream, w_ref[:, 3 * channels :]).astype(BF)
    do_ref[...] = back.reshape(do_ref.shape)
    mix_ref[...] = dot(merge_rows(o_ref[...]).T, upstream) * grad_scale


def backward_kernel(parts, channels, head_size, grad_scale, split, *refs):
    place_ref = refs[0]
    x_refs = refs[1 : 1 + parts]
    (g_ref, do_ref, q_ref, k_ref, v_ref, p_ref, mix_ref, w_ref) = refs[1 + parts : 9 + parts]
    out_refs = refs[9 + parts : 9 + 2 * parts]
    keep_ref, send_ref, dq_ref, dk_ref, dv_ref, dp_ref, ds_ref, total_ref = refs[9 + 2 * parts :]
    frames, rows, cols, _ = q_ref.shape
    tokens = frames * cols
    scaling = head_size ** (-0.5)
    tiles = head_tiles(channels, head_size)
    for row in range(rows):
        for start, width, heads in tiles:
            lanes = slice(start, start + width)
            grads = stack_heads(tile_of(do_ref, row, lanes), heads, head_size)
            span = slice(heads[0] * tokens, (heads[-1] + 1) * tokens)
            dp_ref[row, :, span] = dot(tile_of(v_ref, row, lanes), grads, ((1,), (1,)))
    for row in range(rows):
        for head in range(channels // head_size):
            span = slice(head * tokens, (head + 1) * tokens)
            prob = p_ref[row, :, span]
            d_prob = dp_ref[row, :, span]
            row_dot = jnp.sum(prob * d_prob, axis=0, keepdims=True)
            ds_ref[row, :, span] = (prob * (d_prob - row_dot)).astype(BF)
    for row in range(rows):
        for start, width, heads in tiles:
            lanes = slice(start, start + width)
            span = slice(heads[0] * tokens, (heads[-1] + 1) * tokens)
            d_score = ds_ref[row, :, span]
            queries = stack_heads(tile_of(q_ref, row, lanes), heads, head_size)
            grads = stack_heads(tile_of(do_ref, row, lanes), heads, head_size)
            dq = pick_heads(dot(d_score, tile_of(k_ref, row, lanes), ((0,), (0,))), heads, head_size)
            dk = dot(d_score, queries)
            dv = dot(p_ref[row, :, span].astype(BF), grads)
            for ref, grad in ((dq_ref, dq * scaling), (dk_ref, dk * scaling), (dv_ref, dv)):
                ref[:, row, :, lanes] = grad.astype(BF).reshape(frames, cols, width)
    d_inputs = None
    for place, ref in enumerate((dq_ref, dk_ref, dv_ref)):
        block = slice(place * channels, (place + 1) * channels)
        term = dot(merge_rows(ref[...]), w_ref[:, block])
        d_inputs = term if d_inputs is None else d_inputs + term
    grads = (merge_rows(g_ref[...]).astype(F32) + d_inputs.astype(BF).astype(F32)).astype(BF)
    share = grads.shape[0] // parts
    for step, ref in enumerate(out_refs):
        ref[...] = grads[step * share : (step + 1) * share].reshape(ref.shape)
    latents = jnp.concatenate([merge_rows(ref[...])[:, :channels] for ref in x_refs], axis=0)
    turned = latents.T
    for place, ref in enumerate((dq_ref, dk_ref, dv_ref)):
        block = slice(place * channels, (place + 1) * channels)
        total_ref[block, :] = dot(turned, merge_rows(ref[...])) * grad_scale
    total_ref[3 * channels :, :] = mix_ref[...]
    write_blocks(total_ref, keep_ref, send_ref, place_ref, split)


def place_kernel(parts, *refs):
    place_ref = refs[0]
    part_refs = refs[1 : 1 + parts]
    out_ref = refs[1 + parts]
    rows = part_refs[0].shape[1]
    for step, ref in enumerate(part_refs):
        out_ref[:, pl.ds((place_ref[0] ^ step) * rows, rows)] = ref[...]


def prepare_kernel(parts, *refs):
    place_ref, x_hbm, mask_hbm, dy_hbm = refs[:4]
    x_refs = refs[4 : 4 + parts]
    dy_refs = refs[4 + parts : 4 + 2 * parts]
    edge_refs = refs[4 + 2 * parts : 4 + 3 * parts]
    x_ref, mask_ref, sems = refs[4 + 3 * parts :]
    frames, rows, cols, wide = x_refs[0].shape
    channels = x_ref.shape[-1]
    count = x_ref.shape[1]
    me = place_ref[0]
    moves = [(x_hbm, x_ref), (mask_hbm, mask_ref)]
    for step in range(parts):
        first = (me ^ step) * rows
        for source, size, to in (
            (first, rows, 1),
            (jnp.maximum(first - 1, 0), 1, 0),
            (jnp.minimum(first + rows, count - 1), 1, rows + 1),
        ):
            moves.append(
                (dy_hbm.at[:, pl.ds(source, size)], dy_refs[step].at[:, pl.ds(to, size)])
            )
        row = jnp.where(me == step, count - 1, 0)
        moves.append((dy_hbm.at[:, pl.ds(row, 1)], edge_refs[step]))
    copies = [
        pltpu.make_async_copy(source, target, sems.at[place])
        for place, (source, target) in enumerate(moves)
    ]
    for copy in copies:
        copy.start()
    for copy in copies[:2]:
        copy.wait()
    blank = jnp.zeros((1, wide - channels - cols), F32)
    for step, ref in enumerate(x_refs):
        first = (me ^ step) * rows
        ref[:, :, :, :channels] = x_ref[:, pl.ds(first, rows)]
        for frame in range(frames):
            for row in range(rows):
                line = mask_ref[frame, pl.ds(first + row, 1), :].astype(F32)
                spare = jnp.concatenate([line, blank], axis=1)
                spare = jnp.broadcast_to(spare, (cols, wide - channels))
                ref[frame, row, :, channels:] = spare.astype(BF)
    for copy in copies[2:]:
        copy.wait()


def bias_kernel(head_count, frame_count, cols, *refs):
    place_ref, time_hbm, w_hbm, bias_ref, w_ref, time_ref, sems = refs
    tokens = bias_ref.shape[0]
    all_frames = time_ref.shape[1]
    copies = [
        pltpu.make_async_copy(time_hbm, time_ref, sems.at[0]),
        pltpu.make_async_copy(w_hbm, w_ref, sems.at[1]),
    ]
    for copy in copies:
        copy.start()

    def product(left, right):
        return lax.dot_general(
            left,
            right,
            (((1,), (1,)), ((), ())),
            precision=lax.Precision.HIGHEST,
            preferred_element_type=F32,
        )

    def held(slot):
        far = (slot // (cols * frame_count)) ^ place_ref[0]
        return far * frame_count + (slot // cols) % frame_count

    def index(shape, axis):
        return lax.broadcasted_iota(jnp.int32, shape, axis)

    keys = (tokens, all_frames)
    one_hot = jnp.where(held(index(keys, 0)) == index(keys, 1), 1.0, 0.0).astype(F32)
    square = (tokens, tokens)
    same = index(square, 0) % cols == index(square, 1) % cols
    copies[0].wait()
    by_key = product(one_hot, time_ref[...].reshape(head_count * all_frames, all_frames))
    for head in range(head_count):
        part = by_key[:, head * all_frames : (head + 1) * all_frames]
        spread = jnp.where(same, product(part, one_hot), -1e30)
        bias_ref[:, head * tokens : (head + 1) * tokens] = spread
    copies[1].wait()


def pair_sum_kernel(*refs):
    left_ref, right_ref = refs[:2]
    for step, ref in enumerate(refs[2:]):
        ref[...] = (left_ref[step].astype(F32) + right_ref[step].astype(F32)).astype(BF)


def sum_of(refs):
    total = refs[0][...].astype(F32)
    for ref in refs[1:]:
        total = total + ref[...].astype(F32)
    return total


def spread_sum_kernel(count, *refs):
    total = sum_of(refs[:count])
    for step, ref in enumerate(refs[count:]):
        ref[...] = total[step].astype(ref.dtype)


def scatter_sum_kernel(count, *refs):
    place_ref = refs[0]
    out_refs = refs[1 + count : -1]
    total_ref = refs[-1]
    share = out_refs[0].shape[0]
    total = sum_of(refs[1 : 1 + count])
    if total.shape[0] < total_ref.shape[0]:
        total_ref[...] = jnp.zeros(total_ref.shape, F32)
    total_ref[: total.shape[0], :] = total
    for step, ref in enumerate(out_refs):
        first = pl.multiple_of((place_ref[0] ^ step) * share, 8)
        ref[...] = total_ref[pl.ds(first, share), :].astype(BF)


def plain_sum_kernel(*refs):
    refs[-1][...] = sum_of(refs[:-1]).astype(refs[-1].dtype)


def gather_kernel(parts, *refs):
    place_ref = refs[0]
    out_ref, total_ref = refs[1 + parts :]
    share = refs[1].shape[0]
    for step, ref in enumerate(refs[1 : 1 + parts]):
        first = pl.multiple_of((place_ref[0] ^ step) * share, 8)
        total_ref[pl.ds(first, share), :] = ref[...].astype(F32)
    out_ref[...] = total_ref[: out_ref.shape[0], :]


def call(kernel, outs, args, scratch=(), scalars=False, far=0, flops=0):
    vmem = pl.BlockSpec(memory_space=pltpu.VMEM)
    smem = pl.BlockSpec(memory_space=pltpu.SMEM)
    specs = [vmem] * len(args)
    if scalars:
        specs[0] = smem
    args = list(args)
    for index in range(1, 1 + far):
        specs[index] = pl.BlockSpec(memory_space=pltpu.MemorySpace.HBM)
        args[index] = pltpu.with_memory_space_constraint(args[index], pltpu.MemorySpace.HBM)
    moved = sum(v.size * v.dtype.itemsize for v in list(args) + list(outs))
    return pl.pallas_call(
        kernel,
        out_shape=outs,
        in_specs=specs,
        out_specs=[vmem] * len(outs),
        scratch_shapes=list(scratch),
        cost_estimate=pl.CostEstimate(flops=flops, transcendentals=0, bytes_accessed=moved),
        compiler_params=pltpu.CompilerParams(vmem_limit_bytes=16 * 1024 * 1024),
    )(*args)


def block_size(total, owners):
    size = total // owners
    return size if size % 8 == 0 else None


def pack_blocks(plain, frame_count, height_count, dp_count, me, high, side):
    blocks = plain.reshape(frame_count, height_count, dp_count, -1, plain.shape[-1])
    far = jnp.arange(frame_count) ^ (me if frame_count > 1 else 0)
    blocks = blocks[far][:, jnp.arange(height_count) ^ high]
    blocks = jnp.swapaxes(blocks, 0, 1)
    keep = lax.dynamic_index_in_dim(blocks, side, 2, keepdims=False)
    send = lax.dynamic_index_in_dim(blocks, 1 - side, 2, keepdims=False)
    return keep, send


def like(shape, dtype=BF):
    return jax.ShapeDtypeStruct(tuple(shape), dtype)


def whole_body(clip_latents, out_grad, box_mask, attn_weights, conv_weights, time_bias):
    clips, frame_count, row_count, cols, channels = clip_latents.shape
    head_count, all_frames, _ = time_bias.shape
    head_size = channels // head_count
    parts = lax.axis_size("frame")
    height_count = lax.axis_size("height")
    dp_count = lax.axis_size("dp")
    me = lax.axis_index("frame")
    high = lax.axis_index("height")
    side = lax.axis_index("dp")
    rows = row_count // parts
    assert clips == 1 and dp_count == 2 and rows * parts == row_count
    assert is_pow2(parts) and is_pow2(height_count)
    tokens = all_frames * cols
    pixels = tokens * rows
    place = jnp.stack([me, high, side]).astype(jnp.int32)

    def trades(values, axis):
        return [values[0]] + [
            trade(values[step], axis, step) for step in range(1, lax.axis_size(axis))
        ]

    x = clip_latents[0]
    dy = out_grad[0]
    spare = -channels % LANES
    assert cols <= spare
    wide = like((frame_count, rows, cols, channels + spare))
    blocks = call(
        functools.partial(prepare_kernel, parts),
        [wide] * parts
        + [like((frame_count, rows + 2, cols, channels))] * parts
        + [like((frame_count, 1, cols, channels))] * parts,
        [place, x, box_mask[0], dy],
        scratch=[
            pltpu.VMEM(x.shape, BF),
            pltpu.VMEM(box_mask.shape[1:], jnp.int32),
            pltpu.SemaphoreType.DMA((2 + 4 * parts,)),
        ],
        scalars=True,
        far=3,
    )
    x_parts = trades(blocks[:parts], "frame")

    last = parts - 1
    dy_parts = trades(blocks[parts : 2 * parts], "frame")
    edges = []
    for step in range(parts):
        pairs = []
        for i in range(height_count - 1):
            pairs.append((step * height_count + i, i + 1))
            pairs.append(((last ^ step) * height_count + i + 1, last * height_count + i))
        edges.append(lax.ppermute(blocks[2 * parts + step], ("frame", "height"), pairs))

    bias, attn_turned = call(
        functools.partial(bias_kernel, head_count, frame_count, cols),
        [like((tokens, head_count * tokens), F32), like((channels, 4 * channels))],
        [place, time_bias, attn_weights.T],
        scratch=[pltpu.VMEM(time_bias.shape, F32), pltpu.SemaphoreType.DMA((2,))],
        scalars=True,
        far=2,
    )

    half = like((all_frames, rows, cols, channels))
    square = (rows, tokens, head_count * tokens)
    q, k, v, p, o, y, a = call(
        functools.partial(forward_kernel, parts, channels, head_size),
        [half, half, half, like(square, F32), half, half, half],
        list(x_parts) + [attn_turned, bias],
        scratch=[pltpu.VMEM(square, F32)],
        flops=8 * pixels * channels * channels,
    )

    token_count = pixels * dp_count * parts * height_count
    grad_scale = float(token_count) ** (-0.5)

    def block_outs(total, frames, turn=False):
        size = block_size(total, frames * height_count * dp_count)
        if size is None:
            return None, [like((total, channels)), like((8, channels))]
        block = (channels, size) if turn else (frames, size, channels)
        shape = like((height_count,) + block)
        return (frames, height_count, dp_count, size), [shape, shape]

    def over_height(keep, send):
        got = lax.ppermute(send, "dp", [(0, 1), (1, 0)])
        both = call(pair_sum_kernel, [like(keep.shape[1:])] * height_count, [keep, got])
        return trades(both, "height")

    taps = conv_weights.shape[0]
    split, outs = block_outs(taps, 1, turn=True)
    keep, send, moves = call(
        functools.partial(conv_grad_kernel, parts, grad_scale, split),
        outs + [like((3, all_frames, rows + 2, cols, channels))],
        [place] + dy_parts + edges + [a],
        scratch=[pltpu.VMEM((taps, channels), F32)],
        scalars=True,
        flops=2 * pixels * taps * channels,
    )
    if split is None:
        keep, send = pack_blocks(keep, 1, height_count, dp_count, 0, high, side)
        keep, send = jnp.swapaxes(keep[:, 0], 1, 2), jnp.swapaxes(send[:, 0], 1, 2)
    conv_terms = over_height(keep, send)

    g, do, mix = call(
        functools.partial(upstream_kernel, channels, grad_scale),
        [half, half, like((channels, channels), F32)],
        [moves, y, o, attn_turned, conv_weights.T],
        flops=2 * pixels * taps * channels,
    )
    split, outs = block_outs(4 * channels, parts)
    piece = like((frame_count, rows, cols, channels))
    result = call(
        functools.partial(backward_kernel, parts, channels, head_size, grad_scale, split),
        [piece] * parts + outs,
        [place] + list(x_parts) + [g, do, q, k, v, p, mix, attn_turned],
        scratch=[pltpu.VMEM(half.shape, BF)] * 3
        + [pltpu.VMEM(square, F32), pltpu.VMEM(square, BF)]
        + [pltpu.VMEM((4 * channels, channels), F32)],
        scalars=True,
        flops=2 * pixels * taps * channels,
    )
    grad_parts = [result[0]]
    for step in range(1, parts):
        grad_parts.append(trade(result[step], "frame", step))
    keep, send = result[parts:]
    if split is None:
        keep, send = pack_blocks(keep, parts, height_count, dp_count, me, high, side)
    attn_terms = over_height(keep, send)
    shares = call(
        functools.partial(spread_sum_kernel, height_count),
        [like(keep.shape[2:])] * parts,
        attn_terms,
    )
    shares = trades(shares, "frame")
    grad_attn = call(plain_sum_kernel, [like(keep.shape[2:], F32)], shares)[0]

    size = conv_terms[0].shape[1]
    share = -(-channels // (parts * 8)) * 8
    shares = call(
        functools.partial(scatter_sum_kernel, height_count),
        [like((share, size))] * parts,
        [place] + conv_terms,
        scratch=[pltpu.VMEM((parts * share, size), F32)],
        scalars=True,
    )
    shares = trades(shares, "frame")
    mine = call(plain_sum_kernel, [like((share, size))], shares)[0]
    shares = trades([mine] * parts, "frame")
    grad_conv = call(
        functools.partial(gather_kernel, parts),
        [like((channels, size), F32)],
        [place] + shares,
        scratch=[pltpu.VMEM((parts * share, size), F32)],
        scalars=True,
    )[0].T
    grad_input = call(
        functools.partial(place_kernel, parts),
        [like((frame_count, row_count, cols, channels))],
        [place] + grad_parts,
        scalars=True,
    )[0]
    return (grad_input.reshape(clip_latents.shape), grad_attn, grad_conv)


def solution(mesh):
    in_specs = (
        P("dp", "frame", "height", None, None),
        P("dp", "frame", "height", None, None),
        P("dp", "frame", "height", None),
        P(),
        P(),
        P(),
    )
    out_specs = (
        P("dp", "frame", "height", None, None),
        P(("frame", "height", "dp"), None),
        P(("height", "dp"), None),
    )
    return jax.shard_map(whole_body, mesh=mesh, in_specs=in_specs, out_specs=out_specs, check_vma=False)
```

```python
import functools

import jax
import jax.numpy as jnp
from jax import lax
from jax.experimental import pallas as pl
from jax.experimental.pallas import tpu as pltpu
from jax.sharding import PartitionSpec as P


ground_bias = 2.0
LANES = 128
BF = jnp.bfloat16
F32 = jnp.float32


def dot(left, right, dims=((1,), (0,))):
    return lax.dot_general(left, right, (dims, ((), ())), preferred_element_type=F32)


def is_pow2(count):
    return count & (count - 1) == 0


def peer(index, step, count):
    if is_pow2(count):
        return index ^ step
    return (step - index) % count


def trade(value, axis, step):
    count = lax.axis_size(axis)
    return lax.ppermute(value, axis, [(i, peer(i, step, count)) for i in range(count)])


def sigmoid(value):
    return 1.0 / (1.0 + jnp.exp(-value))


def merge_rows(value):
    return value.reshape(-1, value.shape[-1])


def up_to(count, unit):
    return -(-count // unit) * unit


def packed_rows(count, channels):
    whole, rest = divmod(channels, LANES)
    assert rest <= LANES // 2 and count % 32 == 0
    return count * whole + (count // 2 if rest else 0)


def pack(ref, value):
    count, channels = value.shape
    whole, rest = divmod(channels, LANES)
    for tile in range(whole):
        ref[tile * count : (tile + 1) * count, :] = value[:, tile * LANES : (tile + 1) * LANES]
    if rest:
        half = count // 2
        sides = [value[:half, whole * LANES :], value[half:, whole * LANES :]]
        if 2 * rest < LANES:
            sides.append(jnp.zeros((half, LANES - 2 * rest), value.dtype))
        ref[whole * count : whole * count + half, :] = jnp.concatenate(sides, axis=1)


def unpack(ref, count, channels):
    whole, rest = divmod(channels, LANES)
    tiles = [ref[tile * count : (tile + 1) * count, :] for tile in range(whole)]
    if rest:
        half = ref[whole * count : whole * count + count // 2, :]
        tiles.append(jnp.concatenate([half[:, :rest], half[:, rest : 2 * rest]], axis=0))
    return jnp.concatenate(tiles, axis=1)


def head_tiles(channels, head_size):
    step = max(LANES, head_size)
    tiles = []
    for start in range(0, channels, step):
        width = min(step, channels - start)
        tiles.append((start, width, range(start // head_size, (start + width) // head_size)))
    return tiles


def head_mask(tokens, width, head_size, place):
    lane = lax.broadcasted_iota(jnp.int32, (tokens, width), 1)
    return lane // head_size == place


def stack_heads(tile, heads, head_size):
    if len(heads) == 1:
        return tile
    masks = [head_mask(*tile.shape, head_size, place) for place in range(len(heads))]
    return jnp.concatenate([tile * mask.astype(BF) for mask in masks], axis=0)


def pick_heads(stacked, heads, head_size):
    tokens = stacked.shape[0] // len(heads)
    result = stacked[:tokens]
    for place in range(1, len(heads)):
        mask = head_mask(tokens, stacked.shape[1], head_size, place)
        result = jnp.where(mask, stacked[place * tokens : (place + 1) * tokens], result)
    return result


def tile_of(ref, row, lanes):
    frames, _, cols, _ = ref.shape
    return ref[:, row, :, lanes].reshape(frames * cols, lanes.stop - lanes.start)


def forward_kernel(parts, channels, head_size, *refs):
    x_refs = refs[:parts]
    w_ref, bias_ref = refs[parts : parts + 2]
    x_ref, q_ref, k_ref, v_ref, p_ref, o_ref, y_ref, a_ref, s_ref = refs[parts + 2 :]
    frames, rows, cols, _ = q_ref.shape
    tokens = frames * cols
    head_count = channels // head_size
    count = tokens * rows // parts
    at = packed_rows(count, channels)
    lines = x_refs[0].shape[0] - at
    latents = jnp.concatenate([unpack(ref, count, channels) for ref in x_refs], axis=0)
    x_ref[...] = latents.reshape(x_ref.shape)
    for place, ref in enumerate((q_ref, k_ref, v_ref)):
        block = slice(place * channels, (place + 1) * channels)
        part = dot(latents, w_ref[:, block], ((1,), (1,))).astype(BF)
        ref[...] = part.reshape(ref.shape)
    scaling = head_size ** (-0.5)
    held = jnp.concatenate([ref[at:, :] for ref in x_refs], axis=0)
    lane = lax.broadcasted_iota(jnp.int32, (LANES, tokens), 0)
    column = lax.broadcasted_iota(jnp.int32, (LANES, tokens), 1)
    held = dot(held, jnp.where(lane == column % cols, ground_bias, 0.0).astype(BF)).astype(BF)
    token = lax.broadcasted_iota(jnp.int32, (tokens, parts * lines), 0) // cols
    line = lax.broadcasted_iota(jnp.int32, (tokens, parts * lines), 1)
    part_frames = frames // parts
    first_line = (token // part_frames) * lines + (token % part_frames) * rows
    tiles = head_tiles(channels, head_size)
    for row in range(rows):
        for start, width, heads in tiles:
            lanes = slice(start, start + width)
            queries = stack_heads(tile_of(q_ref, row, lanes), heads, head_size)
            span = slice(heads[0] * tokens, (heads[-1] + 1) * tokens)
            s_ref[row, :, span] = dot(tile_of(k_ref, row, lanes), queries, ((1,), (1,)))
    for row in range(rows):
        mark = dot(jnp.where(line == first_line + row, 1.0, 0.0).astype(BF), held)
        for head in range(head_count):
            span = slice(head * tokens, (head + 1) * tokens)
            score = s_ref[row, :, span] * scaling + (bias_ref[:, span] + mark)
            score = jnp.exp(score - jnp.max(score, axis=0, keepdims=True))
            p_ref[row, :, span] = score * (1.0 / jnp.sum(score, axis=0, keepdims=True))
    for row in range(rows):
        for start, width, heads in tiles:
            lanes = slice(start, start + width)
            span = slice(heads[0] * tokens, (heads[-1] + 1) * tokens)
            out = dot(p_ref[row, :, span].astype(BF), tile_of(v_ref, row, lanes), ((0,), (0,)))
            mixed = pick_heads(out, heads, head_size).astype(BF)
            o_ref[:, row, :, lanes] = mixed.reshape(frames, cols, width)
    mixed = merge_rows(o_ref[...])
    residual = (latents.astype(F32) + dot(mixed, w_ref[:, 3 * channels :], ((1,), (1,)))).astype(BF)
    y_ref[...] = residual.reshape(y_ref.shape)
    value = residual.astype(F32)
    a_ref[...] = (value * sigmoid(value)).astype(BF).reshape(a_ref.shape)


def column_moves(me, dy_refs, edge_refs, move_ref, cols):
    frames, high, _, channels = move_ref.shape
    channels = channels // 3
    parts = len(dy_refs)
    shape = (frames // parts, high, cols, channels)
    blocks = []
    for ref, edge_ref in zip(dy_refs, edge_refs):
        block = unpack(ref, shape[0] * high * cols, channels).reshape(shape)
        edge = edge_ref[...]
        first = jnp.where(me == 0, edge, block[:, :1])
        last = jnp.where(me == parts - 1, edge, block[:, -1:])
        blocks.append(jnp.concatenate([first, block[:, 1:-1], last], axis=1))
    whole = jnp.concatenate(blocks, axis=0)
    wide = merge_rows(whole).astype(F32)
    count = wide.shape[0]
    col = lax.broadcasted_iota(jnp.int32, wide.shape, 0) % cols
    left = jnp.where(col == cols - 1, 0.0, pltpu.roll(wide, count - 1, 0))
    right = jnp.where(col == 0, 0.0, pltpu.roll(wide, 1, 0))
    for place, moved in enumerate((left.astype(BF).reshape(whole.shape), whole)):
        move_ref[:, :, :, place * channels : (place + 1) * channels] = moved
    move_ref[:, :, :, 2 * channels :] = right.astype(BF).reshape(whole.shape)


def rows_of(moves, row_step, rows):
    return merge_rows(moves[:, 1 - row_step : 1 - row_step + rows])


def place_block(both_ref, place_ref, split, block, value):
    frame_count, height_count, dp_count, _ = split
    step = (block // dp_count % height_count) ^ place_ref[1]
    side = (block % dp_count) ^ place_ref[2]
    if frame_count > 1:
        far = (block // (dp_count * height_count)) ^ place_ref[0]
        both_ref[side, step, far] = value
    else:
        both_ref[side, step] = value


def conv_grad_kernel(parts, grad_scale, split, *refs):
    place_ref = refs[0]
    dy_refs = refs[1 : 1 + parts]
    edge_refs = refs[1 + parts : 1 + 2 * parts]
    a_ref, both_ref, send_ref, move_ref, total_ref = refs[1 + 2 * parts :]
    _, rows, cols, channels = a_ref.shape
    column_moves(place_ref[0], dy_refs, edge_refs, move_ref, cols)
    act = merge_rows(a_ref[...]).T
    block = 0
    for line in range(3):
        terms = dot(act, rows_of(move_ref, line - 1, rows)) * grad_scale
        for place in range(3):
            first = (3 * line + place) * channels
            total_ref[first : first + channels, :] = terms[:, place * channels : (place + 1) * channels]
        if split is not None:
            size = split[3]
            while (block + 1) * size <= 3 * (line + 1) * channels:
                value = total_ref[block * size : (block + 1) * size, :].astype(BF).T
                place_block(both_ref, place_ref, split, block, value)
                block += 1
    if split is None:
        both_ref[...] = total_ref[...].astype(BF)
    else:
        send_ref[...] = both_ref[1]


def upstream_kernel(channels, grad_scale, *refs):
    moves, y_ref, o_ref, w_ref, conv_ref, g_ref, do_ref, mix_ref = refs
    rows = g_ref.shape[1]
    delta = None
    for line in range(3):
        taps = [
            conv_ref[:, tap * channels : (tap + 1) * channels]
            for tap in range(3 * line, 3 * line + 3)
        ]
        term = dot(rows_of(moves, line - 1, rows), jnp.concatenate(taps, axis=0))
        delta = term if delta is None else delta + term
    value = merge_rows(y_ref[...]).astype(F32)
    sig = sigmoid(value)
    slope = sig * (1.0 + value * (1.0 - sig))
    dy = merge_rows(moves[:, 1 : 1 + rows, :, channels : 2 * channels]).astype(F32)
    upstream = (dy + slope * delta).astype(BF)
    g_ref[...] = upstream.reshape(g_ref.shape)
    back = dot(upstream, w_ref[:, 3 * channels :]).astype(BF)
    do_ref[...] = back.reshape(do_ref.shape)
    mix_ref[...] = dot(merge_rows(o_ref[...]).T, upstream) * grad_scale


def backward_kernel(parts, channels, head_size, grad_scale, split, *refs):
    place_ref = refs[0]
    (x_ref, g_ref, do_ref, q_ref, k_ref, v_ref, p_ref, mix_ref, w_ref) = refs[1:10]
    out_refs = refs[10 : 10 + parts]
    both_ref, send_ref, dq_ref, dk_ref, dv_ref, dp_ref, ds_ref = refs[10 + parts :]
    frames, rows, cols, _ = q_ref.shape
    tokens = frames * cols
    scaling = head_size ** (-0.5)
    tiles = head_tiles(channels, head_size)
    for row in range(rows):
        for start, width, heads in tiles:
            lanes = slice(start, start + width)
            grads = stack_heads(tile_of(do_ref, row, lanes), heads, head_size)
            span = slice(heads[0] * tokens, (heads[-1] + 1) * tokens)
            dp_ref[row, :, span] = dot(tile_of(v_ref, row, lanes), grads, ((1,), (1,)))
    for row in range(rows):
        for head in range(channels // head_size):
            span = slice(head * tokens, (head + 1) * tokens)
            prob = p_ref[row, :, span]
            d_prob = dp_ref[row, :, span]
            row_dot = jnp.sum(prob * d_prob, axis=0, keepdims=True)
            ds_ref[row, :, span] = (prob * (d_prob - row_dot)).astype(BF)
    for row in range(rows):
        for start, width, heads in tiles:
            lanes = slice(start, start + width)
            span = slice(heads[0] * tokens, (heads[-1] + 1) * tokens)
            d_score = ds_ref[row, :, span]
            queries = stack_heads(tile_of(q_ref, row, lanes), heads, head_size)
            grads = stack_heads(tile_of(do_ref, row, lanes), heads, head_size)
            dq = pick_heads(dot(d_score, tile_of(k_ref, row, lanes), ((0,), (0,))), heads, head_size)
            dk = dot(d_score, queries)
            dv = dot(p_ref[row, :, span].astype(BF), grads)
            for ref, grad in ((dq_ref, dq * scaling), (dk_ref, dk * scaling), (dv_ref, dv)):
                ref[:, row, :, lanes] = grad.astype(BF).reshape(frames, cols, width)
    d_inputs = None
    for place, ref in enumerate((dq_ref, dk_ref, dv_ref)):
        block = slice(place * channels, (place + 1) * channels)
        term = dot(merge_rows(ref[...]), w_ref[:, block])
        d_inputs = term if d_inputs is None else d_inputs + term
    grads = (merge_rows(g_ref[...]).astype(F32) + d_inputs.astype(BF).astype(F32)).astype(BF)
    share = grads.shape[0] // parts
    for step, ref in enumerate(out_refs):
        pack(ref, grads[step * share : (step + 1) * share])
    turned = merge_rows(x_ref[...]).T
    for place, ref in enumerate((dq_ref, dk_ref, dv_ref, mix_ref)):
        if ref is mix_ref:
            total = ref[...]
        else:
            total = dot(turned, merge_rows(ref[...])) * grad_scale
        if split is None:
            both_ref[place * channels : (place + 1) * channels, :] = total.astype(BF)
            continue
        size = split[3]
        for part in range(channels // size):
            block = place * (channels // size) + part
            value = total[part * size : (part + 1) * size].astype(BF)
            place_block(both_ref, place_ref, split, block, value)
    if split is not None:
        send_ref[...] = both_ref[1]


def place_kernel(parts, *refs):
    place_ref = refs[0]
    part_refs = refs[1 : 1 + parts]
    out_ref = refs[1 + parts]
    frames, count, cols, channels = out_ref.shape
    shape = (frames, count // parts, cols, channels)
    for step, ref in enumerate(part_refs):
        block = unpack(ref, frames * shape[1] * cols, channels).reshape(shape)
        out_ref[:, pl.ds((place_ref[0] ^ step) * shape[1], shape[1])] = block


def prepare_kernel(parts, *refs):
    place_ref, x_hbm, mask_hbm, dy_hbm = refs[:4]
    x_refs = refs[4 : 4 + parts]
    dy_refs = refs[4 + parts : 4 + 2 * parts]
    edge_refs = refs[4 + 2 * parts : 4 + 3 * parts]
    x_ref, mask_ref, dy_ref, sems = refs[4 + 3 * parts :]
    frames, count, cols, channels = x_ref.shape
    rows = count // parts
    me = place_ref[0]
    moves = ((x_hbm, x_ref), (mask_hbm, mask_ref), (dy_hbm, dy_ref))
    copies = [
        pltpu.make_async_copy(source, target, sems.at[place])
        for place, (source, target) in enumerate(moves)
    ]
    for copy in copies:
        copy.start()
    for copy in copies[:2]:
        copy.wait()
    at = packed_rows(frames * rows * cols, channels)
    lines = x_refs[0].shape[0] - at
    for step, ref in enumerate(x_refs):
        first = (me ^ step) * rows
        pack(ref, merge_rows(x_ref[:, pl.ds(first, rows)]))
        held = [
            mask_ref[frame, pl.ds(first + row, 1), :].astype(F32)
            for frame in range(frames)
            for row in range(rows)
        ]
        if lines > len(held):
            held.append(jnp.zeros((lines - len(held), cols), F32))
        held = [jnp.concatenate(held, axis=0), jnp.zeros((lines, LANES - cols), F32)]
        ref[at:, :] = jnp.concatenate(held, axis=1).astype(BF)
    copies[2].wait()
    for step, ref in enumerate(dy_refs):
        first = (me ^ step) * rows
        block = [
            dy_ref[:, pl.ds(jnp.maximum(first - 1, 0), 1)],
            dy_ref[:, pl.ds(first, rows)],
            dy_ref[:, pl.ds(jnp.minimum(first + rows, count - 1), 1)],
        ]
        pack(ref, merge_rows(jnp.concatenate(block, axis=1)))
    for step, ref in enumerate(edge_refs):
        row = jnp.where(me == step, count - 1, 0)
        ref[...] = dy_ref[:, pl.ds(row, 1)]


def bias_kernel(head_count, frame_count, cols, *refs):
    place_ref, time_hbm, w_hbm, bias_ref, w_ref, time_ref, sems = refs
    tokens = bias_ref.shape[0]
    all_frames = time_ref.shape[1]
    copies = [
        pltpu.make_async_copy(time_hbm, time_ref, sems.at[0]),
        pltpu.make_async_copy(w_hbm, w_ref, sems.at[1]),
    ]
    for copy in copies:
        copy.start()

    def product(left, right):
        return lax.dot_general(
            left,
            right,
            (((1,), (1,)), ((), ())),
            precision=lax.Precision.HIGHEST,
            preferred_element_type=F32,
        )

    def held(slot):
        far = (slot // (cols * frame_count)) ^ place_ref[0]
        return far * frame_count + (slot // cols) % frame_count

    def index(shape, axis):
        return lax.broadcasted_iota(jnp.int32, shape, axis)

    keys = (tokens, all_frames)
    one_hot = jnp.where(held(index(keys, 0)) == index(keys, 1), 1.0, 0.0).astype(F32)
    square = (tokens, tokens)
    same = index(square, 0) % cols == index(square, 1) % cols
    copies[0].wait()
    by_key = product(one_hot, time_ref[...].reshape(head_count * all_frames, all_frames))
    for head in range(head_count):
        part = by_key[:, head * all_frames : (head + 1) * all_frames]
        spread = jnp.where(same, product(part, one_hot), -1e30)
        bias_ref[:, head * tokens : (head + 1) * tokens] = spread
    copies[1].wait()


def pair_sum_kernel(*refs):
    left_ref, right_ref = refs[:2]
    for step, ref in enumerate(refs[2:]):
        ref[...] = (left_ref[0, step].astype(F32) + right_ref[step].astype(F32)).astype(BF)


def sum_of(refs):
    total = refs[0][...].astype(F32)
    for ref in refs[1:]:
        total = total + ref[...].astype(F32)
    return total


def scatter_sum_kernel(count, *refs):
    place_ref = refs[0]
    out_refs = refs[1 + count : -1]
    total_ref = refs[-1]
    share = out_refs[0].shape[0]
    total = sum_of(refs[1 : 1 + count])
    if total.shape[0] < total_ref.shape[0]:
        total_ref[...] = jnp.zeros(total_ref.shape, F32)
    total_ref[: total.shape[0], :] = total
    for step, ref in enumerate(out_refs):
        first = pl.multiple_of((place_ref[0] ^ step) * share, 8)
        ref[...] = total_ref[pl.ds(first, share), :].astype(BF)


def join_kernel(parts, terms, *refs):
    share_refs = refs[:parts]
    term_refs = refs[parts : parts + terms]
    share, size = share_refs[0].shape
    _, rows, channels = term_refs[0].shape
    mine = sum_of(share_refs).astype(BF)
    total = sum_of(term_refs)
    for step, ref in enumerate(refs[parts + terms :]):
        first = up_to(share, 16)
        ref[:share, :size] = mine
        ref[first : first + rows, :channels] = total[step].astype(BF)


def last_kernel(parts, *refs):
    place_ref = refs[0]
    part_refs = refs[1 : 1 + parts]
    conv_ref, attn_ref, total_ref = refs[1 + parts :]
    channels, size = conv_ref.shape
    share = total_ref.shape[0] // parts
    first = up_to(share, 16)
    attn = None
    for step, ref in enumerate(part_refs):
        at = pl.multiple_of((place_ref[0] ^ step) * share, 8)
        total_ref[pl.ds(at, share), :] = ref[:share, :size].astype(F32)
        block = ref[first:, : attn_ref.shape[1]].astype(F32)
        attn = block if attn is None else attn + block
    conv_ref[...] = total_ref[:channels, :]
    attn_ref[...] = attn


def call(kernel, outs, args, scratch=(), scalars=False, far=0, flops=0):
    vmem = pl.BlockSpec(memory_space=pltpu.VMEM)
    smem = pl.BlockSpec(memory_space=pltpu.SMEM)
    specs = [vmem] * len(args)
    if scalars:
        specs[0] = smem
    args = list(args)
    for index in range(1, 1 + far):
        specs[index] = pl.BlockSpec(memory_space=pltpu.MemorySpace.HBM)
        args[index] = pltpu.with_memory_space_constraint(args[index], pltpu.MemorySpace.HBM)
    moved = sum(v.size * v.dtype.itemsize for v in list(args) + list(outs))
    return pl.pallas_call(
        kernel,
        out_shape=outs,
        in_specs=specs,
        out_specs=[vmem] * len(outs),
        scratch_shapes=list(scratch),
        cost_estimate=pl.CostEstimate(flops=flops, transcendentals=0, bytes_accessed=moved),
        compiler_params=pltpu.CompilerParams(vmem_limit_bytes=16 * 1024 * 1024),
    )(*args)


def block_size(total, owners):
    size = total // owners
    return size if size % 8 == 0 and size * owners == total else None


def pack_blocks(plain, frame_count, height_count, dp_count, me, high, side):
    blocks = plain.reshape(frame_count, height_count, dp_count, -1, plain.shape[-1])
    far = jnp.arange(frame_count) ^ (me if frame_count > 1 else 0)
    blocks = blocks[far][:, jnp.arange(height_count) ^ high]
    blocks = jnp.swapaxes(blocks, 0, 1)
    keep = lax.dynamic_index_in_dim(blocks, side, 2, keepdims=False)
    send = lax.dynamic_index_in_dim(blocks, 1 - side, 2, keepdims=False)
    return keep, send


def like(shape, dtype=BF):
    return jax.ShapeDtypeStruct(tuple(shape), dtype)


def whole_body(clip_latents, out_grad, box_mask, attn_weights, conv_weights, time_bias):
    clips, frame_count, row_count, cols, channels = clip_latents.shape
    head_count, all_frames, _ = time_bias.shape
    head_size = channels // head_count
    parts = lax.axis_size("frame")
    height_count = lax.axis_size("height")
    dp_count = lax.axis_size("dp")
    me = lax.axis_index("frame")
    high = lax.axis_index("height")
    side = lax.axis_index("dp")
    rows = row_count // parts
    assert clips == 1 and dp_count == 2 and rows * parts == row_count
    assert is_pow2(parts) and is_pow2(height_count)
    tokens = all_frames * cols
    pixels = tokens * rows
    place = jnp.stack([me, high, side]).astype(jnp.int32)

    def trades(values, axis):
        return [values[0]] + [
            trade(values[step], axis, step) for step in range(1, lax.axis_size(axis))
        ]

    x = clip_latents[0]
    dy = out_grad[0]
    assert cols <= LANES
    block = frame_count * rows * cols
    lines = up_to(frame_count * rows, 16)
    packed = like((packed_rows(block, channels), LANES))
    blocks = call(
        functools.partial(prepare_kernel, parts),
        [like((packed.shape[0] + lines, LANES))] * parts
        + [like((packed_rows(block + 2 * frame_count * cols, channels), LANES))] * parts
        + [like((frame_count, 1, cols, channels))] * parts,
        [place, x, box_mask[0], dy],
        scratch=[
            pltpu.VMEM(x.shape, BF),
            pltpu.VMEM(box_mask.shape[1:], jnp.int32),
            pltpu.VMEM(dy.shape, BF),
            pltpu.SemaphoreType.DMA((3,)),
        ],
        scalars=True,
        far=3,
    )
    x_parts = trades(blocks[:parts], "frame")

    last = parts - 1
    dy_parts = trades(blocks[parts : 2 * parts], "frame")
    edges = []
    for step in range(parts):
        pairs = []
        for i in range(height_count - 1):
            pairs.append((step * height_count + i, i + 1))
            pairs.append(((last ^ step) * height_count + i + 1, last * height_count + i))
        edges.append(lax.ppermute(blocks[2 * parts + step], ("frame", "height"), pairs))

    bias, attn_turned = call(
        functools.partial(bias_kernel, head_count, frame_count, cols),
        [like((tokens, head_count * tokens), F32), like((channels, 4 * channels))],
        [place, time_bias, attn_weights.T],
        scratch=[pltpu.VMEM(time_bias.shape, F32), pltpu.SemaphoreType.DMA((2,))],
        scalars=True,
        far=2,
    )

    half = like((all_frames, rows, cols, channels))
    square = (rows, tokens, head_count * tokens)
    x_all, q, k, v, p, o, y, a = call(
        functools.partial(forward_kernel, parts, channels, head_size),
        [half, half, half, half, like(square, F32), half, half, half],
        list(x_parts) + [attn_turned, bias],
        scratch=[pltpu.VMEM(square, F32)],
        flops=8 * pixels * channels * channels,
    )

    token_count = pixels * dp_count * parts * height_count
    grad_scale = float(token_count) ** (-0.5)

    def block_outs(total, frames, turn=False):
        size = block_size(total, frames * height_count * dp_count)
        if size is None:
            return None, [like((total, channels)), like((8, channels))]
        block = (channels, size) if turn else (frames, size, channels)
        shape = like((height_count,) + block)
        both = like((dp_count, height_count) + block)
        return (frames, height_count, dp_count, size), [both, shape]

    def over_height(both, send):
        got = lax.ppermute(send, "dp", [(0, 1), (1, 0)])
        terms = call(pair_sum_kernel, [like(both.shape[2:])] * height_count, [both, got])
        return trades(terms, "height")

    taps = conv_weights.shape[0]
    split, outs = block_outs(taps, 1, turn=True)
    both, send, moves = call(
        functools.partial(conv_grad_kernel, parts, grad_scale, split),
        outs + [like((all_frames, rows + 2, cols, 3 * channels))],
        [place] + dy_parts + edges + [a],
        scratch=[pltpu.VMEM((taps, channels), F32)],
        scalars=True,
        flops=2 * pixels * taps * channels,
    )
    if split is None:
        both, send = pack_blocks(both, 1, height_count, dp_count, 0, high, side)
        both, send = jnp.swapaxes(both[None, :, 0], 2, 3), jnp.swapaxes(send[:, 0], 1, 2)
    conv_terms = over_height(both, send)

    g, do, mix = call(
        functools.partial(upstream_kernel, channels, grad_scale),
        [half, half, like((channels, channels), F32)],
        [moves, y, o, attn_turned, conv_weights.T],
        flops=2 * pixels * taps * channels,
    )
    split, outs = block_outs(4 * channels, parts)
    result = call(
        functools.partial(backward_kernel, parts, channels, head_size, grad_scale, split),
        [packed] * parts + outs,
        [place, x_all, g, do, q, k, v, p, mix, attn_turned],
        scratch=[pltpu.VMEM(half.shape, BF)] * 3
        + [pltpu.VMEM(square, F32), pltpu.VMEM(square, BF)],
        scalars=True,
        flops=2 * pixels * taps * channels,
    )
    grad_parts = [result[0]]
    for step in range(1, parts):
        grad_parts.append(trade(result[step], "frame", step))
    both, send = result[parts:]
    if split is None:
        both, send = pack_blocks(both, parts, height_count, dp_count, me, high, side)
        both = both[None]
    attn_terms = over_height(both, send)
    size = conv_terms[0].shape[1]
    share = -(-channels // (parts * 8)) * 8
    shares = call(
        functools.partial(scatter_sum_kernel, height_count),
        [like((share, size))] * parts,
        [place] + conv_terms,
        scratch=[pltpu.VMEM((parts * share, size), F32)],
        scalars=True,
    )
    shares = trades(shares, "frame")
    rows_out = send.shape[2]
    joint = like((up_to(share, 16) + rows_out, max(size, channels)))
    joined = call(
        functools.partial(join_kernel, parts, height_count),
        [joint] * parts,
        shares + attn_terms,
    )
    joined = trades(joined, "frame")
    grad_conv, grad_attn = call(
        functools.partial(last_kernel, parts),
        [like((channels, size), F32), like((rows_out, channels), F32)],
        [place] + joined,
        scratch=[pltpu.VMEM((parts * share, size), F32)],
        scalars=True,
    )
    grad_input = call(
        functools.partial(place_kernel, parts),
        [like((frame_count, row_count, cols, channels))],
        [place] + grad_parts,
        scalars=True,
    )[0]
    return (grad_input.reshape(clip_latents.shape), grad_attn, grad_conv.T)


def solution(mesh):
    in_specs = (
        P("dp", "frame", "height", None, None),
        P("dp", "frame", "height", None, None),
        P("dp", "frame", "height", None),
        P(),
        P(),
        P(),
    )
    out_specs = (
        P("dp", "frame", "height", None, None),
        P(("frame", "height", "dp"), None),
        P(("height", "dp"), None),
    )
    return jax.shard_map(whole_body, mesh=mesh, in_specs=in_specs, out_specs=out_specs, check_vma=False)
```

```python
import functools

import jax
import jax.numpy as jnp
from jax import lax
from jax.experimental import pallas as pl
from jax.experimental.pallas import tpu as pltpu
from jax.sharding import PartitionSpec as P


ground_bias = 2.0
LANES = 128
BF = jnp.bfloat16
F32 = jnp.float32


def dot(left, right, dims=((1,), (0,))):
    return lax.dot_general(left, right, (dims, ((), ())), preferred_element_type=F32)


def is_pow2(count):
    return count & (count - 1) == 0


def peer(index, step, count):
    if is_pow2(count):
        return index ^ step
    return (step - index) % count


def trade(value, axis, step):
    count = lax.axis_size(axis)
    return lax.ppermute(value, axis, [(i, peer(i, step, count)) for i in range(count)])


def sigmoid(value):
    return 1.0 / (1.0 + jnp.exp(-value))


def merge_rows(value):
    return value.reshape(-1, value.shape[-1])


def up_to(count, unit):
    return -(-count // unit) * unit


def packed_rows(count, channels):
    whole, rest = divmod(channels, LANES)
    assert rest <= LANES // 2 and count % 32 == 0
    return count * whole + (count // 2 if rest else 0)


def pack(ref, value):
    count, channels = value.shape
    whole, rest = divmod(channels, LANES)
    for tile in range(whole):
        ref[tile * count : (tile + 1) * count, :] = value[:, tile * LANES : (tile + 1) * LANES]
    if rest:
        half = count // 2
        sides = [value[:half, whole * LANES :], value[half:, whole * LANES :]]
        if 2 * rest < LANES:
            sides.append(jnp.zeros((half, LANES - 2 * rest), value.dtype))
        ref[whole * count : whole * count + half, :] = jnp.concatenate(sides, axis=1)


def unpack(ref, count, channels):
    whole, rest = divmod(channels, LANES)
    tiles = [ref[tile * count : (tile + 1) * count, :] for tile in range(whole)]
    if rest:
        half = ref[whole * count : whole * count + count // 2, :]
        tiles.append(jnp.concatenate([half[:, :rest], half[:, rest : 2 * rest]], axis=0))
    return jnp.concatenate(tiles, axis=1)


def head_tiles(channels, head_size):
    step = max(LANES, head_size)
    tiles = []
    for start in range(0, channels, step):
        width = min(step, channels - start)
        tiles.append((start, width, range(start // head_size, (start + width) // head_size)))
    return tiles


def head_mask(tokens, width, head_size, place):
    lane = lax.broadcasted_iota(jnp.int32, (tokens, width), 1)
    return lane // head_size == place


def stack_heads(tile, heads, head_size):
    if len(heads) == 1:
        return tile
    masks = [head_mask(*tile.shape, head_size, place) for place in range(len(heads))]
    return jnp.concatenate([tile * mask.astype(BF) for mask in masks], axis=0)


def pick_heads(stacked, heads, head_size):
    tokens = stacked.shape[0] // len(heads)
    result = stacked[:tokens]
    for place in range(1, len(heads)):
        mask = head_mask(tokens, stacked.shape[1], head_size, place)
        result = jnp.where(mask, stacked[place * tokens : (place + 1) * tokens], result)
    return result


def tile_of(ref, row, lanes):
    frames, _, cols, _ = ref.shape
    return ref[:, row, :, lanes].reshape(frames * cols, lanes.stop - lanes.start)


def forward_kernel(parts, channels, head_size, *refs):
    x_refs = refs[:parts]
    w_ref, bias_ref = refs[parts : parts + 2]
    x_ref, q_ref, k_ref, v_ref, p_ref, o_ref, y_ref, a_ref, s_ref = refs[parts + 2 :]
    frames, rows, cols, _ = q_ref.shape
    tokens = frames * cols
    head_count = channels // head_size
    count = tokens * rows // parts
    at = packed_rows(count, channels)
    lines = x_refs[0].shape[0] - at
    latents = jnp.concatenate([unpack(ref, count, channels) for ref in x_refs], axis=0)
    x_ref[...] = latents.reshape(x_ref.shape)
    for place, ref in enumerate((q_ref, k_ref, v_ref)):
        block = slice(place * channels, (place + 1) * channels)
        part = dot(latents, w_ref[:, block], ((1,), (1,))).astype(BF)
        ref[...] = part.reshape(ref.shape)
    scaling = head_size ** (-0.5)
    held = jnp.concatenate([ref[at:, :] for ref in x_refs], axis=0)
    lane = lax.broadcasted_iota(jnp.int32, (LANES, tokens), 0)
    column = lax.broadcasted_iota(jnp.int32, (LANES, tokens), 1)
    held = dot(held, jnp.where(lane == column % cols, ground_bias, 0.0).astype(BF)).astype(BF)
    token = lax.broadcasted_iota(jnp.int32, (tokens, parts * lines), 0) // cols
    line = lax.broadcasted_iota(jnp.int32, (tokens, parts * lines), 1)
    part_frames = frames // parts
    first_line = (token // part_frames) * lines + (token % part_frames) * rows
    tiles = head_tiles(channels, head_size)
    for row in range(rows):
        for start, width, heads in tiles:
            lanes = slice(start, start + width)
            queries = stack_heads(tile_of(q_ref, row, lanes), heads, head_size)
            span = slice(heads[0] * tokens, (heads[-1] + 1) * tokens)
            s_ref[row, :, span] = dot(tile_of(k_ref, row, lanes), queries, ((1,), (1,)))
    for row in range(rows):
        mark = dot(jnp.where(line == first_line + row, 1.0, 0.0).astype(BF), held)
        for head in range(head_count):
            span = slice(head * tokens, (head + 1) * tokens)
            score = s_ref[row, :, span] * scaling + (bias_ref[:, span] + mark)
            score = jnp.exp(score - jnp.max(score, axis=0, keepdims=True))
            p_ref[row, :, span] = score * (1.0 / jnp.sum(score, axis=0, keepdims=True))
    for row in range(rows):
        for start, width, heads in tiles:
            lanes = slice(start, start + width)
            span = slice(heads[0] * tokens, (heads[-1] + 1) * tokens)
            out = dot(p_ref[row, :, span].astype(BF), tile_of(v_ref, row, lanes), ((0,), (0,)))
            mixed = pick_heads(out, heads, head_size).astype(BF)
            o_ref[:, row, :, lanes] = mixed.reshape(frames, cols, width)
    mixed = merge_rows(o_ref[...])
    residual = (latents.astype(F32) + dot(mixed, w_ref[:, 3 * channels :], ((1,), (1,)))).astype(BF)
    y_ref[...] = residual.reshape(y_ref.shape)
    value = residual.astype(F32)
    a_ref[...] = (value * sigmoid(value)).astype(BF).reshape(a_ref.shape)


def column_moves(dy_refs, move_ref, cols):
    frames, high, _, channels = move_ref.shape
    channels = channels // 3
    parts = len(dy_refs)
    shape = (frames // parts, high, cols, channels)
    blocks = [unpack(ref, shape[0] * high * cols, channels).reshape(shape) for ref in dy_refs]
    whole = jnp.concatenate(blocks, axis=0)
    wide = merge_rows(whole).astype(F32)
    count = wide.shape[0]
    col = lax.broadcasted_iota(jnp.int32, wide.shape, 0) % cols
    left = jnp.where(col == cols - 1, 0.0, pltpu.roll(wide, count - 1, 0))
    right = jnp.where(col == 0, 0.0, pltpu.roll(wide, 1, 0))
    for place, moved in enumerate((left.astype(BF).reshape(whole.shape), whole)):
        move_ref[:, :, :, place * channels : (place + 1) * channels] = moved
    move_ref[:, :, :, 2 * channels :] = right.astype(BF).reshape(whole.shape)


def rows_of(moves, row_step, rows):
    return merge_rows(moves[:, 1 - row_step : 1 - row_step + rows])


def place_block(both_ref, place_ref, split, block, value):
    frame_count, height_count, dp_count, _ = split
    step = (block // dp_count % height_count) ^ place_ref[1]
    side = (block % dp_count) ^ place_ref[2]
    if frame_count > 1:
        far = (block // (dp_count * height_count)) ^ place_ref[0]
        both_ref[side, step, far] = value
    else:
        both_ref[side, step] = value


def conv_grad_kernel(parts, grad_scale, split, *refs):
    place_ref = refs[0]
    dy_refs = refs[1 : 1 + parts]
    a_ref, both_ref, send_ref, move_ref, total_ref = refs[1 + parts :]
    _, rows, cols, channels = a_ref.shape
    column_moves(dy_refs, move_ref, cols)
    act = merge_rows(a_ref[...]).T
    block = 0
    for line in range(3):
        terms = dot(act, rows_of(move_ref, line - 1, rows)) * grad_scale
        for place in range(3):
            first = (3 * line + place) * channels
            total_ref[first : first + channels, :] = terms[:, place * channels : (place + 1) * channels]
        if split is not None:
            size = split[3]
            while (block + 1) * size <= 3 * (line + 1) * channels:
                value = total_ref[block * size : (block + 1) * size, :].astype(BF).T
                place_block(both_ref, place_ref, split, block, value)
                block += 1
    if split is None:
        both_ref[...] = total_ref[...].astype(BF)
    else:
        send_ref[...] = both_ref[1]


def upstream_kernel(channels, grad_scale, *refs):
    moves, y_ref, o_ref, w_ref, conv_ref, g_ref, do_ref, mix_ref = refs
    rows = g_ref.shape[1]
    delta = None
    for line in range(3):
        taps = [
            conv_ref[:, tap * channels : (tap + 1) * channels]
            for tap in range(3 * line, 3 * line + 3)
        ]
        term = dot(rows_of(moves, line - 1, rows), jnp.concatenate(taps, axis=0))
        delta = term if delta is None else delta + term
    value = merge_rows(y_ref[...]).astype(F32)
    sig = sigmoid(value)
    slope = sig * (1.0 + value * (1.0 - sig))
    dy = merge_rows(moves[:, 1 : 1 + rows, :, channels : 2 * channels]).astype(F32)
    upstream = (dy + slope * delta).astype(BF)
    g_ref[...] = upstream.reshape(g_ref.shape)
    back = dot(upstream, w_ref[:, 3 * channels :]).astype(BF)
    do_ref[...] = back.reshape(do_ref.shape)
    mix_ref[...] = dot(merge_rows(o_ref[...]).T, upstream) * grad_scale


def backward_kernel(parts, channels, head_size, grad_scale, split, *refs):
    place_ref = refs[0]
    (x_ref, g_ref, do_ref, q_ref, k_ref, v_ref, p_ref, mix_ref, w_ref) = refs[1:10]
    out_refs = refs[10 : 10 + parts]
    both_ref, send_ref, dq_ref, dk_ref, dv_ref, dp_ref, ds_ref = refs[10 + parts :]
    frames, rows, cols, _ = q_ref.shape
    tokens = frames * cols
    scaling = head_size ** (-0.5)
    tiles = head_tiles(channels, head_size)
    for row in range(rows):
        for start, width, heads in tiles:
            lanes = slice(start, start + width)
            grads = stack_heads(tile_of(do_ref, row, lanes), heads, head_size)
            span = slice(heads[0] * tokens, (heads[-1] + 1) * tokens)
            dp_ref[row, :, span] = dot(tile_of(v_ref, row, lanes), grads, ((1,), (1,)))
    for row in range(rows):
        for head in range(channels // head_size):
            span = slice(head * tokens, (head + 1) * tokens)
            prob = p_ref[row, :, span]
            d_prob = dp_ref[row, :, span]
            row_dot = jnp.sum(prob * d_prob, axis=0, keepdims=True)
            ds_ref[row, :, span] = (prob * (d_prob - row_dot)).astype(BF)
    for row in range(rows):
        for start, width, heads in tiles:
            lanes = slice(start, start + width)
            span = slice(heads[0] * tokens, (heads[-1] + 1) * tokens)
            d_score = ds_ref[row, :, span]
            queries = stack_heads(tile_of(q_ref, row, lanes), heads, head_size)
            grads = stack_heads(tile_of(do_ref, row, lanes), heads, head_size)
            dq = pick_heads(dot(d_score, tile_of(k_ref, row, lanes), ((0,), (0,))), heads, head_size)
            dk = dot(d_score, queries)
            dv = dot(p_ref[row, :, span].astype(BF), grads)
            for ref, grad in ((dq_ref, dq * scaling), (dk_ref, dk * scaling), (dv_ref, dv)):
                ref[:, row, :, lanes] = grad.astype(BF).reshape(frames, cols, width)
    d_inputs = None
    for place, ref in enumerate((dq_ref, dk_ref, dv_ref)):
        block = slice(place * channels, (place + 1) * channels)
        term = dot(merge_rows(ref[...]), w_ref[:, block])
        d_inputs = term if d_inputs is None else d_inputs + term
    grads = (merge_rows(g_ref[...]).astype(F32) + d_inputs.astype(BF).astype(F32)).astype(BF)
    share = grads.shape[0] // parts
    for step, ref in enumerate(out_refs):
        pack(ref, grads[step * share : (step + 1) * share])
    turned = merge_rows(x_ref[...]).T
    for place, ref in enumerate((dq_ref, dk_ref, dv_ref, mix_ref)):
        if ref is mix_ref:
            total = ref[...]
        else:
            total = dot(turned, merge_rows(ref[...])) * grad_scale
        if split is None:
            both_ref[place * channels : (place + 1) * channels, :] = total.astype(BF)
            continue
        size = split[3]
        for part in range(channels // size):
            block = place * (channels // size) + part
            value = total[part * size : (part + 1) * size].astype(BF)
            place_block(both_ref, place_ref, split, block, value)
    if split is not None:
        send_ref[...] = both_ref[1]


def place_kernel(parts, *refs):
    place_ref = refs[0]
    part_refs = refs[1 : 1 + parts]
    out_ref = refs[1 + parts]
    frames, count, cols, channels = out_ref.shape
    shape = (frames, count // parts, cols, channels)
    for step, ref in enumerate(part_refs):
        block = unpack(ref, frames * shape[1] * cols, channels).reshape(shape)
        out_ref[:, pl.ds((place_ref[0] ^ step) * shape[1], shape[1])] = block


def prepare_kernel(parts, *refs):
    place_ref, x_hbm, mask_hbm, dy_hbm = refs[:4]
    x_refs = refs[4 : 4 + parts]
    dy_ref, one_ref, two_ref, x_ref, mask_ref, sems = refs[4 + parts :]
    frames, count, cols, channels = x_ref.shape
    rows = count // parts
    me = place_ref[0]
    moves = ((x_hbm, x_ref), (mask_hbm, mask_ref), (dy_hbm, dy_ref))
    copies = [
        pltpu.make_async_copy(source, target, sems.at[place])
        for place, (source, target) in enumerate(moves)
    ]
    for copy in copies:
        copy.start()
    for copy in copies[:2]:
        copy.wait()
    at = packed_rows(frames * rows * cols, channels)
    lines = x_refs[0].shape[0] - at
    for step, ref in enumerate(x_refs):
        first = (me ^ step) * rows
        pack(ref, merge_rows(x_ref[:, pl.ds(first, rows)]))
        held = [
            mask_ref[frame, pl.ds(first + row, 1), :].astype(F32)
            for frame in range(frames)
            for row in range(rows)
        ]
        if lines > len(held):
            held.append(jnp.zeros((lines - len(held), cols), F32))
        held = [jnp.concatenate(held, axis=0), jnp.zeros((lines, LANES - cols), F32)]
        ref[at:, :] = jnp.concatenate(held, axis=1).astype(BF)
    copies[2].wait()
    odd = place_ref[1] % 2
    one_ref[...] = dy_ref[:, pl.ds((1 - odd) * (count - 1), 1)]
    two_ref[...] = dy_ref[:, pl.ds(odd * (count - 1), 1)]


def halo_kernel(parts, *refs):
    place_ref, dy_ref, one_ref, two_ref = refs[:4]
    count = dy_ref.shape[1]
    rows = count // parts
    odd = place_ref[1] % 2 == 1
    low = jnp.where(odd, one_ref[...], two_ref[...])
    top = jnp.where(odd, two_ref[...], one_ref[...])
    for step, ref in enumerate(refs[4:]):
        first = (place_ref[0] ^ step) * rows
        above = dy_ref[:, pl.ds(jnp.maximum(first - 1, 0), 1)]
        below = dy_ref[:, pl.ds(jnp.minimum(first + rows, count - 1), 1)]
        block = [
            jnp.where(first == 0, low, above),
            dy_ref[:, pl.ds(first, rows)],
            jnp.where(first + rows == count, top, below),
        ]
        pack(ref, merge_rows(jnp.concatenate(block, axis=1)))


def bias_kernel(head_count, frame_count, cols, *refs):
    place_ref, time_hbm, w_hbm, bias_ref, w_ref, time_ref, sems = refs
    tokens = bias_ref.shape[0]
    all_frames = time_ref.shape[1]
    copies = [
        pltpu.make_async_copy(time_hbm, time_ref, sems.at[0]),
        pltpu.make_async_copy(w_hbm, w_ref, sems.at[1]),
    ]
    for copy in copies:
        copy.start()

    def product(left, right):
        return lax.dot_general(
            left,
            right,
            (((1,), (1,)), ((), ())),
            precision=lax.Precision.HIGHEST,
            preferred_element_type=F32,
        )

    def held(slot):
        far = (slot // (cols * frame_count)) ^ place_ref[0]
        return far * frame_count + (slot // cols) % frame_count

    def index(shape, axis):
        return lax.broadcasted_iota(jnp.int32, shape, axis)

    keys = (tokens, all_frames)
    one_hot = jnp.where(held(index(keys, 0)) == index(keys, 1), 1.0, 0.0).astype(F32)
    square = (tokens, tokens)
    same = index(square, 0) % cols == index(square, 1) % cols
    copies[0].wait()
    by_key = product(one_hot, time_ref[...].reshape(head_count * all_frames, all_frames))
    for head in range(head_count):
        part = by_key[:, head * all_frames : (head + 1) * all_frames]
        spread = jnp.where(same, product(part, one_hot), -1e30)
        bias_ref[:, head * tokens : (head + 1) * tokens] = spread
    copies[1].wait()


def pair_sum_kernel(*refs):
    left_ref, right_ref = refs[:2]
    for step, ref in enumerate(refs[2:]):
        ref[...] = (left_ref[0, step].astype(F32) + right_ref[step].astype(F32)).astype(BF)


def sum_of(refs):
    total = refs[0][...].astype(F32)
    for ref in refs[1:]:
        total = total + ref[...].astype(F32)
    return total


def scatter_sum_kernel(count, *refs):
    place_ref = refs[0]
    term_refs = refs[1 : 1 + count]
    out_refs = refs[1 + count : -1]
    total_ref = refs[-1]
    share = out_refs[0].shape[0]
    rows = term_refs[0].shape[0]
    if share * len(out_refs) == rows and share % 16 == 0:
        for step, ref in enumerate(out_refs):
            first = pl.multiple_of((place_ref[0] ^ step) * share, 16)
            ref[...] = sum_of([term.at[pl.ds(first, share)] for term in term_refs]).astype(BF)
        return
    total_ref[...] = jnp.zeros(total_ref.shape, F32)
    total_ref[:rows, :] = sum_of(term_refs)
    for step, ref in enumerate(out_refs):
        first = pl.multiple_of((place_ref[0] ^ step) * share, 8)
        ref[...] = total_ref[pl.ds(first, share), :].astype(BF)


def join_kernel(parts, terms, *refs):
    share_refs = refs[:parts]
    term_refs = refs[parts : parts + terms]
    share, size = share_refs[0].shape
    _, rows, channels = term_refs[0].shape
    mine = sum_of(share_refs).astype(BF)
    total = sum_of(term_refs)
    for step, ref in enumerate(refs[parts + terms :]):
        first = up_to(share, 16)
        ref[:share, :size] = mine
        ref[first : first + rows, :channels] = total[step].astype(BF)


def last_kernel(parts, *refs):
    place_ref = refs[0]
    part_refs = refs[1 : 1 + parts]
    conv_ref, attn_ref, total_ref = refs[1 + parts :]
    channels, size = conv_ref.shape
    share = total_ref.shape[0] // parts
    first = up_to(share, 16)
    attn = None
    for step, ref in enumerate(part_refs):
        at = pl.multiple_of((place_ref[0] ^ step) * share, 8)
        total_ref[pl.ds(at, share), :] = ref[:share, :size].astype(F32)
        block = ref[first:, : attn_ref.shape[1]].astype(F32)
        attn = block if attn is None else attn + block
    conv_ref[...] = total_ref[:channels, :]
    attn_ref[...] = attn


def call(kernel, outs, args, scratch=(), scalars=False, far=0, flops=0):
    vmem = pl.BlockSpec(memory_space=pltpu.VMEM)
    smem = pl.BlockSpec(memory_space=pltpu.SMEM)
    specs = [vmem] * len(args)
    if scalars:
        specs[0] = smem
    args = list(args)
    for index in range(1, 1 + far):
        specs[index] = pl.BlockSpec(memory_space=pltpu.MemorySpace.HBM)
        args[index] = pltpu.with_memory_space_constraint(args[index], pltpu.MemorySpace.HBM)
    moved = sum(v.size * v.dtype.itemsize for v in list(args) + list(outs))
    return pl.pallas_call(
        kernel,
        out_shape=outs,
        in_specs=specs,
        out_specs=[vmem] * len(outs),
        scratch_shapes=list(scratch),
        cost_estimate=pl.CostEstimate(flops=flops, transcendentals=0, bytes_accessed=moved),
        compiler_params=pltpu.CompilerParams(vmem_limit_bytes=16 * 1024 * 1024),
    )(*args)


def block_size(total, owners):
    size = total // owners
    return size if size % 8 == 0 and size * owners == total else None


def pack_blocks(plain, frame_count, height_count, dp_count, me, high, side):
    blocks = plain.reshape(frame_count, height_count, dp_count, -1, plain.shape[-1])
    far = jnp.arange(frame_count) ^ (me if frame_count > 1 else 0)
    blocks = blocks[far][:, jnp.arange(height_count) ^ high]
    blocks = jnp.swapaxes(blocks, 0, 1)
    keep = lax.dynamic_index_in_dim(blocks, side, 2, keepdims=False)
    send = lax.dynamic_index_in_dim(blocks, 1 - side, 2, keepdims=False)
    return keep, send


def like(shape, dtype=BF):
    return jax.ShapeDtypeStruct(tuple(shape), dtype)


def whole_body(clip_latents, out_grad, box_mask, attn_weights, conv_weights, time_bias):
    clips, frame_count, row_count, cols, channels = clip_latents.shape
    head_count, all_frames, _ = time_bias.shape
    head_size = channels // head_count
    parts = lax.axis_size("frame")
    height_count = lax.axis_size("height")
    dp_count = lax.axis_size("dp")
    me = lax.axis_index("frame")
    high = lax.axis_index("height")
    side = lax.axis_index("dp")
    rows = row_count // parts
    assert clips == 1 and dp_count == 2 and rows * parts == row_count
    assert is_pow2(parts) and is_pow2(height_count) and height_count > 1
    tokens = all_frames * cols
    pixels = tokens * rows
    place = jnp.stack([me, high, side]).astype(jnp.int32)

    def trades(values, axis):
        result = [values[0]]
        for step in range(1, lax.axis_size(axis)):
            result.append(trade(values[step], axis, step))
        return result

    x = clip_latents[0]
    dy = out_grad[0]
    assert cols <= LANES
    block = frame_count * rows * cols
    lines = up_to(frame_count * rows, 16)
    packed = like((packed_rows(block, channels), LANES))
    blocks = call(
        functools.partial(prepare_kernel, parts),
        [like((packed.shape[0] + lines, LANES))] * parts
        + [like(dy.shape)]
        + [like((frame_count, 1, cols, channels))] * 2,
        [place, x, box_mask[0], dy],
        scratch=[
            pltpu.VMEM(x.shape, BF),
            pltpu.VMEM(box_mask.shape[1:], jnp.int32),
            pltpu.SemaphoreType.DMA((3,)),
        ],
        scalars=True,
        far=3,
    )
    x_parts = trades(blocks[:parts], "frame")
    dy, one, two = blocks[parts:]
    swaps = [(i, i + 1) for i in range(1, height_count - 1, 2)]
    two = lax.ppermute(two, "height", swaps + [(j, i) for i, j in swaps])
    one = trade(one, "height", 1)
    blocks = call(
        functools.partial(halo_kernel, parts),
        [like((packed_rows(block + 2 * frame_count * cols, channels), LANES))] * parts,
        [place, dy, one, two],
        scalars=True,
    )
    dy_parts = trades(blocks, "frame")

    bias, attn_turned = call(
        functools.partial(bias_kernel, head_count, frame_count, cols),
        [like((tokens, head_count * tokens), F32), like((channels, 4 * channels))],
        [place, time_bias, attn_weights.T],
        scratch=[pltpu.VMEM(time_bias.shape, F32), pltpu.SemaphoreType.DMA((2,))],
        scalars=True,
        far=2,
    )

    half = like((all_frames, rows, cols, channels))
    square = (rows, tokens, head_count * tokens)
    x_all, q, k, v, p, o, y, a = call(
        functools.partial(forward_kernel, parts, channels, head_size),
        [half, half, half, half, like(square, F32), half, half, half],
        list(x_parts) + [attn_turned, bias],
        scratch=[pltpu.VMEM(square, F32)],
        flops=8 * pixels * channels * channels,
    )

    token_count = pixels * dp_count * parts * height_count
    grad_scale = float(token_count) ** (-0.5)

    def block_outs(total, frames, turn=False):
        size = block_size(total, frames * height_count * dp_count)
        if size is None:
            return None, [like((total, channels)), like((8, channels))]
        block = (channels, size) if turn else (frames, size, channels)
        shape = like((height_count,) + block)
        both = like((dp_count, height_count) + block)
        return (frames, height_count, dp_count, size), [both, shape]

    def over_height(both, send):
        got = lax.ppermute(send, "dp", [(0, 1), (1, 0)])
        terms = call(pair_sum_kernel, [like(both.shape[2:])] * height_count, [both, got])
        return trades(terms, "height")

    taps = conv_weights.shape[0]
    split, outs = block_outs(taps, 1, turn=True)
    both, send, moves = call(
        functools.partial(conv_grad_kernel, parts, grad_scale, split),
        outs + [like((all_frames, rows + 2, cols, 3 * channels))],
        [place] + dy_parts + [a],
        scratch=[pltpu.VMEM((taps, channels), F32)],
        scalars=True,
        flops=2 * pixels * taps * channels,
    )
    if split is None:
        both, send = pack_blocks(both, 1, height_count, dp_count, 0, high, side)
        both, send = jnp.swapaxes(both[None, :, 0], 2, 3), jnp.swapaxes(send[:, 0], 1, 2)
    conv_terms = over_height(both, send)

    g, do, mix = call(
        functools.partial(upstream_kernel, channels, grad_scale),
        [half, half, like((channels, channels), F32)],
        [moves, y, o, attn_turned, conv_weights.T],
        flops=2 * pixels * taps * channels,
    )
    split, outs = block_outs(4 * channels, parts)
    result = call(
        functools.partial(backward_kernel, parts, channels, head_size, grad_scale, split),
        [packed] * parts + outs,
        [place, x_all, g, do, q, k, v, p, mix, attn_turned],
        scratch=[pltpu.VMEM(half.shape, BF)] * 3
        + [pltpu.VMEM(square, F32), pltpu.VMEM(square, BF)],
        scalars=True,
        flops=2 * pixels * taps * channels,
    )
    grad_parts = trades(result[:parts], "frame")
    both, send = result[parts:]
    if split is None:
        both, send = pack_blocks(both, parts, height_count, dp_count, me, high, side)
        both = both[None]
    attn_terms = over_height(both, send)
    size = conv_terms[0].shape[1]
    share = -(-channels // (parts * 8)) * 8
    shares = call(
        functools.partial(scatter_sum_kernel, height_count),
        [like((share, size))] * parts,
        [place] + conv_terms,
        scratch=[pltpu.VMEM((parts * share, size), F32)],
        scalars=True,
    )
    shares = trades(shares, "frame")
    rows_out = send.shape[2]
    joint = like((up_to(share, 16) + rows_out, max(size, channels)))
    joined = call(
        functools.partial(join_kernel, parts, height_count),
        [joint] * parts,
        shares + attn_terms,
    )
    joined = trades(joined, "frame")
    grad_conv, grad_attn = call(
        functools.partial(last_kernel, parts),
        [like((channels, size), F32), like((rows_out, channels), F32)],
        [place] + joined,
        scratch=[pltpu.VMEM((parts * share, size), F32)],
        scalars=True,
    )
    grad_input = call(
        functools.partial(place_kernel, parts),
        [like((frame_count, row_count, cols, channels))],
        [place] + grad_parts,
        scalars=True,
    )[0]
    return (grad_input.reshape(clip_latents.shape), grad_attn, grad_conv.T)


def solution(mesh):
    in_specs = (
        P("dp", "frame", "height", None, None),
        P("dp", "frame", "height", None, None),
        P("dp", "frame", "height", None),
        P(),
        P(),
        P(),
    )
    out_specs = (
        P("dp", "frame", "height", None, None),
        P(("frame", "height", "dp"), None),
        P(("height", "dp"), None),
    )
    return jax.shard_map(whole_body, mesh=mesh, in_specs=in_specs, out_specs=out_specs, check_vma=False)
```
